512 devices in a mesh: row: 32 (over y, x), col: 16 (over z, core).
Axes of the slice: x: 4, y: 8, z: 8, core: 2. Of those that a mesh axis runs over, the one named last changes fastest.
Arguments:
- weights: bfloat16 [8192, 8192], P('row', 'col'), may hold values from 0.0099487305 to 1
- tile_mask: int32 [64, 64], P('row', 'col'), may hold values from 0 to 1, as said below
Outputs:
- flow: float32 [8192, 8192], P('row', 'col')
The draws below stay inside these ranges and needn't reach their ends.
Inputs may be any that keep to these rules, and one draw needn't show every extreme that they name: `tile_mask`: each column of tiles holds exactly 8 ones, the diagonal tile among them.
All inputs are finite; a program needn't handle non-finite values.
Results may differ from the reference program's by a relative error of at most 0.00095.
Values may be sent and summed in bfloat16 or wider, within the bound.
No kernel may reach another device: no remote copies, remote signals or barrier semaphores. Data moves between devices by JAX's collectives and lax.ppermute only.
A program may use at most 64 MiB of HBM per device.

```python
import math
import jax
import jax.numpy as jnp
from jax import lax

TILE = 128
KEEP = 8
NODES = 8192
TILES = 64


def draw_tile_mask(key, part):
    noise = jax.random.randint(key, (TILES, TILES), 0, 1 << 20)
    row_index = lax.broadcasted_iota(jnp.int32, (TILES, TILES), 0)
    col_index = lax.broadcasted_iota(jnp.int32, (TILES, TILES), 1)
    scores = noise * TILES + row_index
    scores = jnp.where(row_index == col_index, jnp.int32(1 << 30), scores)
    ordered = jnp.sort(scores, axis=0)
    cutoff = ordered[TILES - KEEP, :]
    return (scores >= cutoff[None, :]).astype(jnp.int32)


def levels(key, dims, shards, least, top_value):
    loudness, own = 1.0, jax.random.fold_in(key, 6)
    for axis_at, blocks in shards:
        steps = jnp.exp(jax.random.uniform(jax.random.fold_in(own, axis_at), (blocks,), jnp.float32, least / len(shards), top_value / len(shards)))
        loudness = loudness * jnp.repeat(steps, dims[axis_at] // blocks).reshape([-1 if axis == axis_at else 1 for axis in range(len(dims))])
    return loudness


def setup_inputs(seed: int = 0) -> dict:
    seeds = jax.random.split(jax.random.key(seed), 3)
    return {
        "weights": jnp.clip(jnp.exp(math.log(1.0) - 4.61031033 * jax.random.uniform(seeds[0], (NODES, NODES), jnp.float32) ** levels(seeds[0], (NODES, NODES), ((0, 32), (1, 16)), -0.2, 0.2)), 0.0099487305, 1.0).astype(jnp.bfloat16),
        "tile_mask": draw_tile_mask(jax.random.fold_in(seeds[2], 71), 0),
    }


def reference(weights, tile_mask):
    spread = jnp.repeat(jnp.repeat(tile_mask, TILE, axis=0), TILE, axis=1).astype(jnp.float32)
    masked = weights.astype(jnp.float32) * spread
    degree = jnp.sum(masked, axis=0)
    markov = (masked / degree[None, :]).astype(jnp.bfloat16)
    expanded = jnp.dot(markov, markov, preferred_element_type=jnp.float32)
    inflated = expanded * expanded
    mass = jnp.sum(inflated, axis=0)
    return inflated / mass[None, :] * NODES
```

```python
import jax
import jax.numpy as jnp
from jax import lax
from jax.experimental import pallas as pl
from jax.experimental.pallas import tpu as pltpu
from jax.sharding import Mesh, PartitionSpec as P

KEEP = 8
TILE = 128
SLICE = 16
NY, NX, NZ, NC = 8, 4, 8, 2
ROWS = NY * NX
ROW = ("y", "x")
F32, BF16 = jnp.float32, jnp.bfloat16
VMEM = pl.BlockSpec(memory_space=pltpu.VMEM)
SMEM = pl.BlockSpec(memory_space=pltpu.SMEM)


def exchange(blocks, axis):
    return lax.all_to_all(blocks, axis, split_axis=0, concat_axis=0, tiled=True)


def to_everyone(block, axis, size):
    return exchange(jnp.broadcast_to(block, (size, *block.shape)), axis)


def swap_cores(block):
    return lax.ppermute(block, "core", [(0, 1), (1, 0)])


def split3(v):
    parts = []
    for _ in range(3):
        part = v.astype(BF16)
        parts.append(part)
        v = v - part.astype(F32)
    return parts


def prepare_kernel(mask_ref, w_ref, upper_ref, lower_ref, sent_ref):
    lane = lax.broadcasted_iota(jnp.int32, (1, TILE), 1)
    on_row = jnp.zeros((1, TILE), F32)
    sums = []
    for c in range(4):
        cols = pl.ds(c * TILE, TILE)
        total = jnp.zeros((1, TILE), F32)
        for t in range(2):
            panel = (upper_ref, lower_ref)[t]
            on = mask_ref[t, c].astype(F32)
            on_row = jnp.where(lane == t * 4 + c, on, on_row)
            tile = w_ref[pl.ds(t * TILE, TILE), cols].astype(F32) * on
            total = total + jnp.sum(tile, axis=0, keepdims=True)
            tile = tile.astype(BF16)
            panel[:, cols] = tile
            for e in range(8):
                sent_ref[8 * c + e, pl.ds(t * SLICE, SLICE)] = tile[e * SLICE : (e + 1) * SLICE]
        sums.append(split3(total))
    rows = [sums[c][p].astype(F32) for p in range(3) for c in range(4)]
    extra = jnp.concatenate([*rows, on_row, jnp.zeros((3, TILE), F32)], axis=0).astype(BF16)
    for d in range(ROWS):
        sent_ref[d, pl.ds(2 * SLICE, SLICE)] = extra


def prepare(mask, weights):
    return pl.pallas_call(
        prepare_kernel,
        out_shape=(
            jax.ShapeDtypeStruct((TILE, 4 * TILE), BF16),
            jax.ShapeDtypeStruct((TILE, 4 * TILE), BF16),
            jax.ShapeDtypeStruct((ROWS, 3 * SLICE, TILE), BF16),
        ),
        in_specs=[SMEM, VMEM],
        out_specs=(VMEM,) * 3,
        name="prepare",
    )(mask, weights)


def place_kernel(own_ref, ids_ref, got_ref, lower_ref, placed_ref, extended_ref):
    extra = jnp.zeros((SLICE, TILE), F32)
    for r in range(ROWS):
        extra = extra + got_ref[r, pl.ds(2 * SLICE, SLICE)].astype(F32)
    degree = extra[0:4] + (extra[4:8] + extra[8:12])
    own = own_ref[0]
    mine = jnp.zeros((1, TILE), F32)
    for c in range(4):
        mine = jnp.where(own == c, degree[c : c + 1], mine)
    extended_ref[pl.ds(0, TILE)] = lower_ref[...]
    for c in range(4):
        parts = [part.astype(F32) for part in split3(degree[c : c + 1])]
        block = jnp.concatenate([*parts, jnp.zeros((13, TILE), F32)], axis=0)
        extended_ref[pl.ds(TILE, SLICE), pl.ds(c * TILE, TILE)] = block.astype(BF16)
    for s in range(KEEP):
        k = ids_ref[s, own]
        start = pl.multiple_of((k % 2) * SLICE, SLICE)
        tile = got_ref[k // 2, pl.ds(start, SLICE)].astype(F32)
        placed_ref[s] = (tile / mine).astype(BF16)


def place(own, ids, got, lower):
    return pl.pallas_call(
        place_kernel,
        out_shape=(
            jax.ShapeDtypeStruct((KEEP, SLICE, TILE), BF16),
            jax.ShapeDtypeStruct((TILE + SLICE, 4 * TILE), BF16),
        ),
        in_specs=[SMEM, SMEM, VMEM, VMEM],
        out_specs=(VMEM, VMEM),
        name="place",
    )(own, ids, got, lower)


def expand_kernel(core_ref, ids_ref, upper_ref, upper_o_ref, lower_ref, lower_o_ref, right_ref, out_ref, mass_ref):
    core = core_ref[0]
    for c in range(4):
        cols = pl.ds(c * TILE, TILE)
        totals = [jnp.zeros((TILE, TILE), F32), jnp.zeros((TILE, TILE), F32)]
        for s in range(KEEP):
            k = ids_ref[s, c]
            column = k // 4
            z = column // 2
            ours = column % 2 == core
            inside = pl.ds(pl.multiple_of((k % 4) * TILE, TILE), TILE)
            parts = jnp.where(
                ours,
                lower_ref[z, pl.ds(TILE, SLICE), inside].astype(F32),
                lower_o_ref[z, pl.ds(TILE, SLICE), inside].astype(F32),
            )
            inverse = 1.0 / (parts[0:1] + (parts[1:2] + parts[2:3]))
            right = right_ref[pl.ds(8 * c, 8), s].reshape(TILE, TILE)
            for t in range(2):
                mine, other = ((upper_ref, upper_o_ref), (lower_ref, lower_o_ref))[t]
                left = jnp.where(
                    ours,
                    mine[z, pl.ds(0, TILE), inside].astype(F32),
                    other[z, pl.ds(0, TILE), inside].astype(F32),
                )
                left = (left * inverse).astype(BF16)
                totals[t] = totals[t] + jnp.dot(left, right, preferred_element_type=F32)
        part = jnp.zeros((1, TILE), F32)
        for t in range(2):
            squared = totals[t] * totals[t]
            out_ref[pl.ds(t * TILE, TILE), cols] = squared
            part = part + jnp.sum(squared, axis=0, keepdims=True)
        mass_ref[:, cols] = part


def expand(core, ids, upper, upper_o, lower, lower_o, right):
    return pl.pallas_call(
        expand_kernel,
        out_shape=(
            jax.ShapeDtypeStruct((2 * TILE, 4 * TILE), F32),
            jax.ShapeDtypeStruct((1, 4 * TILE), F32),
        ),
        in_specs=[SMEM, SMEM] + [VMEM] * 5,
        out_specs=(VMEM, VMEM),
        name="expand",
    )(core, ids, upper, upper_o, lower, lower_o, right)


def on_device(weights, tile_mask):
    upper, lower, sent = prepare(tile_mask, weights)
    upper_z = lax.all_gather(upper, "z")
    got = exchange(sent, ROW)
    there = (got[:, 44, :8].reshape(64, 4) > 0).astype(jnp.int32)
    rank = jnp.cumsum(there, axis=0) - there
    tile_ids = lax.broadcasted_iota(jnp.int32, (KEEP, 64, 4), 1)
    ranks = lax.broadcasted_iota(jnp.int32, (KEEP, 64, 4), 0)
    chosen = (there == 1)[None] & (rank[None] == ranks)
    ids = jnp.sum(jnp.where(chosen, tile_ids, 0), axis=1)
    own = (lax.axis_index("y") // 2).reshape(1)
    core = lax.axis_index("core")
    placed, lower = place(own, ids, got, lower)
    lower_z = lax.all_gather(lower, "z")
    right = to_everyone(placed, ROW, ROWS)
    inflated, mass = expand(
        core.reshape(1), ids, upper_z, swap_cores(upper_z), lower_z, swap_cores(lower_z), right
    )
    mass = to_everyone(mass, ROW, ROWS).sum(axis=0)
    nodes = 64 * TILE
    return inflated * (nodes / mass)


def solution(mesh):
    split = Mesh(mesh.devices.reshape(NY, NX, NZ, NC), ("y", "x", "z", "core"))
    placed = P(ROW, ("z", "core"))
    return jax.shard_map(
        on_device, mesh=split, in_specs=(placed, placed), out_specs=placed, check_vma=False
    )
```

```python
import jax
import jax.numpy as jnp
from jax import lax
from jax.experimental import pallas as pl
from jax.experimental.pallas import tpu as pltpu
from jax.sharding import Mesh, PartitionSpec as P

KEEP = 8
TILE = 128
SLICE = 16
NY, NX, NZ, NC = 8, 4, 8, 2
ROWS = NY * NX
ROW = ("y", "x")
F32, BF16 = jnp.float32, jnp.bfloat16
VMEM = pl.BlockSpec(memory_space=pltpu.VMEM)
SMEM = pl.BlockSpec(memory_space=pltpu.SMEM)


def exchange(blocks, axis):
    return lax.all_to_all(blocks, axis, split_axis=0, concat_axis=0, tiled=True)


def split3(v):
    parts = []
    for _ in range(3):
        part = v.astype(BF16)
        parts.append(part)
        v = v - part.astype(F32)
    return parts


def prepare_kernel(mask_ref, w_ref, panel_ref, sent_ref):
    lane = lax.broadcasted_iota(jnp.int32, (1, TILE), 1)
    on_row = jnp.zeros((1, TILE), F32)
    sums = []
    for c in range(4):
        cols = pl.ds(c * TILE, TILE)
        total = jnp.zeros((1, TILE), F32)
        for t in range(2):
            on = mask_ref[t, c].astype(F32)
            on_row = jnp.where(lane == t * 4 + c, on, on_row)
            tile = w_ref[pl.ds(t * TILE, TILE), cols].astype(F32) * on
            total = total + jnp.sum(tile, axis=0, keepdims=True)
            tile = tile.astype(BF16)
            panel_ref[pl.ds(t * TILE, TILE), cols] = tile
            for e in range(8):
                sent_ref[8 * c + e, pl.ds(t * SLICE, SLICE)] = tile[e * SLICE : (e + 1) * SLICE]
        sums.append(split3(total))
    rows = [sums[c][p].astype(F32) for p in range(3) for c in range(4)]
    extra = jnp.concatenate([*rows, on_row, jnp.zeros((3, TILE), F32)], axis=0).astype(BF16)
    for d in range(ROWS):
        sent_ref[d, pl.ds(2 * SLICE, SLICE)] = extra


def prepare(mask, weights):
    return pl.pallas_call(
        prepare_kernel,
        out_shape=(
            jax.ShapeDtypeStruct((2 * TILE, 4 * TILE), BF16),
            jax.ShapeDtypeStruct((ROWS, 3 * SLICE, TILE), BF16),
        ),
        in_specs=[SMEM, VMEM],
        out_specs=(VMEM,) * 2,
        name="prepare",
    )(mask, weights)


def place_kernel(own_ref, ids_ref, got_ref, placed_ref, degree_ref):
    extra = jnp.zeros((SLICE, TILE), F32)
    for r in range(ROWS):
        extra = extra + got_ref[r, pl.ds(2 * SLICE, SLICE)].astype(F32)
    degree = extra[0:4] + (extra[4:8] + extra[8:12])
    degree_ref[...] = degree
    own = own_ref[0]
    mine = jnp.zeros((1, TILE), F32)
    for c in range(4):
        mine = jnp.where(own == c, degree[c : c + 1], mine)
    for s in range(KEEP):
        k = ids_ref[s, own]
        start = pl.multiple_of((k % 2) * SLICE, SLICE)
        tile = got_ref[k // 2, pl.ds(start, SLICE)].astype(F32)
        tile = (tile / mine).astype(BF16)
        for r in range(ROWS):
            placed_ref[r, s] = tile


def place(own, ids, got):
    return pl.pallas_call(
        place_kernel,
        out_shape=(
            jax.ShapeDtypeStruct((ROWS, KEEP, SLICE, TILE), BF16),
            jax.ShapeDtypeStruct((4, TILE), F32),
        ),
        in_specs=[SMEM, SMEM, VMEM],
        out_specs=(VMEM, VMEM),
        name="place",
    )(own, ids, got)


def expand_kernel(col_ref, ids_ref, degree_ref, panel_ref, right_ref, out_ref, mass_ref):
    col = col_ref[0]
    for c in range(4):
        cols = pl.ds(c * TILE, TILE)
        total = jnp.zeros((2 * TILE, TILE), F32)
        for s in range(KEEP):
            k = ids_ref[s, c]
            inside = pl.ds(pl.multiple_of((k % 4) * TILE, TILE), TILE)
            inverse = 1.0 / degree_ref[(k // 4) ^ col, pl.ds(k % 4, 1), :]
            right = right_ref[pl.ds(8 * c, 8), s].reshape(TILE, TILE)
            left = (panel_ref[k // 4, :, inside].astype(F32) * inverse).astype(BF16)
            total = total + jnp.dot(left, right, preferred_element_type=F32)
        total = total * total
        out_ref[:, cols] = total
        part = jnp.sum(total, axis=0, keepdims=True)
        for r in range(ROWS):
            mass_ref[r, :, cols] = part


def expand(col, ids, degree, panel, right):
    return pl.pallas_call(
        expand_kernel,
        out_shape=(
            jax.ShapeDtypeStruct((2 * TILE, 4 * TILE), F32),
            jax.ShapeDtypeStruct((ROWS, 1, 4 * TILE), F32),
        ),
        in_specs=[SMEM, SMEM] + [VMEM] * 3,
        out_specs=(VMEM, VMEM),
        name="expand",
    )(col, ids, degree, panel, right)


def spread(block, axis, size):
    step = 1
    while step < size:
        other = lax.ppermute(block, axis, [(i, i ^ step) for i in range(size)])
        block = jnp.concatenate([block, other])
        step *= 2
    return block


def on_device(weights, tile_mask):
    masked, sent = prepare(tile_mask, weights)
    panel = lax.all_gather(masked, ("z", "core"))
    got = exchange(sent, ROW)
    there = (got[:, 44, :8].reshape(64, 4) > 0).astype(jnp.int32)
    rank = jnp.cumsum(there, axis=0) - there
    tile_ids = lax.broadcasted_iota(jnp.int32, (KEEP, 64, 4), 1)
    ranks = lax.broadcasted_iota(jnp.int32, (KEEP, 64, 4), 0)
    chosen = (there == 1)[None] & (rank[None] == ranks)
    ids = jnp.sum(jnp.where(chosen, tile_ids, 0), axis=1)
    own = (lax.axis_index("y") // 2).reshape(1)
    col = lax.axis_index(("z", "core")).reshape(1)
    placed, degree = place(own, ids, got)
    right = exchange(placed, ROW)
    degree = spread(spread(degree[None], "core", NC), "z", NZ)
    inflated, mass = expand(col, ids, degree, panel, right)
    mass = exchange(mass, ROW).sum(axis=0)
    nodes = 64 * TILE
    return inflated * (nodes / mass)


def solution(mesh):
    split = Mesh(mesh.devices.reshape(NY, NX, NZ, NC), ("y", "x", "z", "core"))
    placed = P(ROW, ("z", "core"))
    return jax.shard_map(
        on_device, mesh=split, in_specs=(placed, placed), out_specs=placed, check_vma=False
    )
```

```python
import jax
import jax.numpy as jnp
from jax import lax
from jax.experimental import pallas as pl
from jax.experimental.pallas import tpu as pltpu
from jax.sharding import Mesh, PartitionSpec as P

KEEP = 8
TILE = 128
SLICE = 16
NY, NX, NZ, NC = 8, 4, 8, 2
ROWS = NY * NX
ROW = ("y", "x")
F32, BF16 = jnp.float32, jnp.bfloat16
VMEM = pl.BlockSpec(memory_space=pltpu.VMEM)
SMEM = pl.BlockSpec(memory_space=pltpu.SMEM)


def exchange(blocks, axis):
    return lax.all_to_all(blocks, axis, split_axis=0, concat_axis=0, tiled=True)


def near(x):
    return pltpu.with_memory_space_constraint(x, pltpu.VMEM)


def split3(v):
    parts = []
    for _ in range(3):
        part = v.astype(BF16)
        parts.append(part)
        v = v - part.astype(F32)
    return parts


def prepare_kernel(mask_ref, w_ref, panel_ref, sent_ref):
    lane = lax.broadcasted_iota(jnp.int32, (1, TILE), 1)
    packed = jnp.zeros((1, TILE), F32)
    sums, masks = [], []
    for c in range(4):
        cols = pl.ds(c * TILE, TILE)
        total = jnp.zeros((1, TILE), F32)
        for t in range(2):
            on = mask_ref[t, c].astype(F32)
            masks.append(jnp.full((1, TILE), on, F32))
            packed = jnp.where(lane == t * 4 + c, on, packed)
            tile = w_ref[pl.ds(t * TILE, TILE), cols].astype(F32) * on
            total = total + jnp.sum(tile, axis=0, keepdims=True)
            tile = tile.astype(BF16)
            panel_ref[pl.ds(t * TILE, TILE), cols] = tile
            for e in range(8):
                sent_ref[8 * c + e, pl.ds(t * SLICE, SLICE)] = tile[e * SLICE : (e + 1) * SLICE]
        sums.append(split3(total))
    rows = [sums[c][p].astype(F32) for p in range(3) for c in range(4)]
    for c in range(4):
        extra = jnp.concatenate([*rows, packed, packed, *masks[2 * c : 2 * c + 2]], axis=0).astype(BF16)
        for e in range(8):
            sent_ref[8 * c + e, pl.ds(2 * SLICE, SLICE)] = extra


def prepare(mask, weights):
    return pl.pallas_call(
        prepare_kernel,
        out_shape=(
            jax.ShapeDtypeStruct((2 * TILE, 4 * TILE), BF16),
            pltpu.VMEM((ROWS, 3 * SLICE, TILE), BF16),
        ),
        in_specs=[SMEM, VMEM],
        out_specs=(VMEM,) * 2,
        name="prepare",
    )(mask, weights)


def place_kernel(own_ref, got_ref, placed_ref, degree_ref, slot_ref):
    total = jnp.zeros((SLICE, TILE), F32)
    masks = []
    for r in range(ROWS):
        extra = got_ref[r, pl.ds(2 * SLICE, SLICE)].astype(F32)
        total = total + extra
        masks.append(extra[14:16])
    degree = total[0:4] + (total[4:8] + total[8:12])
    degree_ref[...] = degree
    there = jnp.concatenate(masks, axis=0)
    above = lax.broadcasted_iota(jnp.int32, (64, 64), 0) > lax.broadcasted_iota(jnp.int32, (64, 64), 1)
    rank = jnp.dot(above.astype(BF16), there.astype(BF16), preferred_element_type=F32)
    slot_ref[...] = jnp.where(there > 0, rank, -1.0)
    own = own_ref[0]
    mine = jnp.zeros((1, TILE), F32)
    for c in range(4):
        mine = jnp.where(own == c, degree[c : c + 1], mine)
    kept = [jnp.zeros((SLICE, TILE), F32) for _ in range(KEEP)]
    for k in range(64):
        tile = got_ref[k // 2, pl.ds((k % 2) * SLICE, SLICE)].astype(F32)
        slot = jnp.broadcast_to(slot_ref[pl.ds(k, 1)], (SLICE, TILE))
        for s in range(KEEP):
            kept[s] = jnp.where(slot == s, tile, kept[s])
    for s in range(KEEP):
        tile = (kept[s] / mine).astype(BF16)
        for r in range(ROWS):
            placed_ref[r, s] = tile


def place(own, got):
    return pl.pallas_call(
        place_kernel,
        out_shape=(
            pltpu.VMEM((ROWS, KEEP, SLICE, TILE), BF16),
            pltpu.VMEM((4, TILE), F32),
        ),
        in_specs=[SMEM, VMEM],
        out_specs=(VMEM, VMEM),
        scratch_shapes=[pltpu.VMEM((64, TILE), F32)],
        name="place",
    )(own, near(got))


def expand_kernel(ids_ref, degree_ref, panel_ref, right_ref, out_ref, mass_ref):
    for c in range(4):
        cols = pl.ds(c * TILE, TILE)
        total = jnp.zeros((2 * TILE, TILE), F32)
        for pair in range(KEEP // 2):
            lefts, rights = [], []
            for s in (2 * pair, 2 * pair + 1):
                k = ids_ref[s, c]
                inside = pl.ds(pl.multiple_of((k % 4) * TILE, TILE), TILE)
                inverse = 1.0 / degree_ref[k // 4, pl.ds(k % 4, 1), :]
                lefts.append((panel_ref[k // 4, :, inside].astype(F32) * inverse).astype(BF16))
                rights.append(right_ref[pl.ds(8 * c, 8), s].reshape(TILE, TILE))
            total = total + jnp.dot(
                jnp.concatenate(lefts, axis=1),
                jnp.concatenate(rights, axis=0),
                preferred_element_type=F32,
            )
        total = total * total
        out_ref[:, cols] = total
        part = jnp.sum(total, axis=0, keepdims=True)
        for r in range(ROWS):
            mass_ref[r, :, cols] = part


def expand(ids, degree, panel, right):
    return pl.pallas_call(
        expand_kernel,
        out_shape=(
            pltpu.VMEM((2 * TILE, 4 * TILE), F32),
            pltpu.VMEM((ROWS, 1, 4 * TILE), F32),
        ),
        in_specs=[SMEM] + [VMEM] * 3,
        out_specs=(VMEM, VMEM),
        name="expand",
    )(ids, degree, panel, near(right))


def scale_kernel(inflated_ref, mass_ref, flow_ref):
    mass = jnp.sum(mass_ref[...], axis=0)
    flow_ref[...] = inflated_ref[...] * (64.0 * TILE / mass)


def scale(inflated, mass):
    return pl.pallas_call(
        scale_kernel,
        out_shape=jax.ShapeDtypeStruct((2 * TILE, 4 * TILE), F32),
        in_specs=[VMEM, VMEM],
        out_specs=VMEM,
        name="scale",
    )(near(inflated), near(mass))


def on_device(weights, tile_mask):
    masked, sent = prepare(tile_mask, weights)
    panel = lax.all_gather(masked, ("z", "core"))
    got = exchange(sent, ROW)
    own = (lax.axis_index("y") // 2).reshape(1)
    placed, degree = place(own, got)
    right = exchange(placed, ROW)
    degree = lax.all_gather(degree, ("z", "core"))
    there = (got[:, 44, :8].reshape(64, 4) > 0).astype(jnp.int32)
    rank = jnp.cumsum(there, axis=0) - there
    tile_ids = lax.broadcasted_iota(jnp.int32, (KEEP, 64, 4), 1)
    ranks = lax.broadcasted_iota(jnp.int32, (KEEP, 64, 4), 0)
    chosen = (there == 1)[None] & (rank[None] == ranks)
    ids = jnp.sum(jnp.where(chosen, tile_ids, 0), axis=1)
    inflated, mass = expand(ids, degree, panel, right)
    return scale(inflated, exchange(mass, ROW))


def solution(mesh):
    split = Mesh(mesh.devices.reshape(NY, NX, NZ, NC), ("y", "x", "z", "core"))
    placed = P(ROW, ("z", "core"))
    return jax.shard_map(
        on_device, mesh=split, in_specs=(placed, placed), out_specs=placed, check_vma=False
    )
```

```python
import jax
import jax.numpy as jnp
from jax import lax
from jax.experimental import pallas as pl
from jax.experimental.pallas import tpu as pltpu
from jax.sharding import Mesh, PartitionSpec as P

KEEP = 8
TILE = 128
SLICE = 16
NY, NX, NZ, NC = 8, 4, 8, 2
ROWS = NY * NX
ROW = ("y", "x")
F32, BF16, I16 = jnp.float32, jnp.bfloat16, jnp.int16
UNIT = 16384.0
VMEM = pl.BlockSpec(memory_space=pltpu.VMEM)
SMEM = pl.BlockSpec(memory_space=pltpu.SMEM)


def exchange(blocks, axis):
    return lax.all_to_all(blocks, axis, split_axis=0, concat_axis=0, tiled=True)


def near(x):
    return pltpu.with_memory_space_constraint(x, pltpu.VMEM)


def split3(v):
    parts = []
    for _ in range(3):
        part = v.astype(BF16)
        parts.append(part)
        v = v - part.astype(F32)
    return parts


def prepare_kernel(mask_ref, w_ref, panel_ref, sent_ref):
    lane = lax.broadcasted_iota(jnp.int32, (1, TILE), 1)
    packed = jnp.zeros((1, TILE), F32)
    sums, masks = [], []
    for c in range(4):
        cols = pl.ds(c * TILE, TILE)
        total = jnp.zeros((1, TILE), F32)
        for t in range(2):
            on = mask_ref[t, c].astype(F32)
            masks.append(jnp.full((1, TILE), on, F32))
            packed = jnp.where(lane == t * 4 + c, on, packed)
            tile = w_ref[pl.ds(t * TILE, TILE), cols].astype(F32) * on
            total = total + jnp.sum(tile, axis=0, keepdims=True)
            panel_ref[pl.ds(t * TILE, TILE), cols] = (tile * UNIT).astype(jnp.int32).astype(I16)
            tile = tile.astype(BF16)
            for e in range(8):
                sent_ref[8 * c + e, pl.ds(t * SLICE, SLICE)] = tile[e * SLICE : (e + 1) * SLICE]
        sums.append(split3(total))
    rows = [sums[c][p].astype(F32) for p in range(3) for c in range(4)]
    for c in range(4):
        extra = jnp.concatenate([*rows, packed, packed, *masks[2 * c : 2 * c + 2]], axis=0).astype(BF16)
        for e in range(8):
            sent_ref[8 * c + e, pl.ds(2 * SLICE, SLICE)] = extra


def prepare(mask, weights):
    return pl.pallas_call(
        prepare_kernel,
        out_shape=(
            pltpu.VMEM((2 * TILE, 4 * TILE), I16),
            pltpu.VMEM((ROWS, 3 * SLICE, TILE), BF16),
        ),
        in_specs=[SMEM, VMEM],
        out_specs=(VMEM,) * 2,
        name="prepare",
    )(mask, weights)


def place_kernel(own_ref, got_ref, panel_ref, placed_ref, full_ref, slot_ref):
    total = jnp.zeros((SLICE, TILE), F32)
    masks = []
    for r in range(ROWS):
        extra = got_ref[r, pl.ds(2 * SLICE, SLICE)].astype(F32)
        total = total + extra
        masks.append(extra[14:16])
    degree = total[0:4] + (total[4:8] + total[8:12])
    full_ref[pl.ds(0, 2 * TILE)] = panel_ref[...]
    for c in range(4):
        high = jnp.floor(degree[c : c + 1] * 16.0)
        low = (degree[c : c + 1] * 16.0 - high) * UNIT
        rows = jnp.concatenate([high, low, jnp.zeros((6, TILE), F32)], axis=0)
        full_ref[pl.ds(2 * TILE, 8), pl.ds(c * TILE, TILE)] = rows.astype(jnp.int32).astype(I16)
    there = jnp.concatenate(masks, axis=0)
    above = lax.broadcasted_iota(jnp.int32, (64, 64), 0) > lax.broadcasted_iota(jnp.int32, (64, 64), 1)
    rank = jnp.dot(above.astype(BF16), there.astype(BF16), preferred_element_type=F32)
    slot_ref[...] = jnp.where(there > 0, rank, -1.0)
    own = own_ref[0]
    mine = jnp.zeros((1, TILE), F32)
    for c in range(4):
        mine = jnp.where(own == c, degree[c : c + 1], mine)
    kept = [jnp.zeros((SLICE, TILE), F32) for _ in range(KEEP)]
    for k in range(64):
        tile = got_ref[k // 2, pl.ds((k % 2) * SLICE, SLICE)].astype(F32)
        slot = jnp.broadcast_to(slot_ref[pl.ds(k, 1)], (SLICE, TILE))
        for s in range(KEEP):
            kept[s] = jnp.where(slot == s, tile, kept[s])
    for s in range(KEEP):
        tile = (kept[s] / mine).astype(BF16)
        for r in range(ROWS):
            placed_ref[r, s] = tile


def place(own, got, panel):
    return pl.pallas_call(
        place_kernel,
        out_shape=(
            pltpu.VMEM((ROWS, KEEP, SLICE, TILE), BF16),
            pltpu.VMEM((2 * TILE + 8, 4 * TILE), I16),
        ),
        in_specs=[SMEM, VMEM, VMEM],
        out_specs=(VMEM, VMEM),
        scratch_shapes=[pltpu.VMEM((64, TILE), F32)],
        name="place",
    )(own, near(got), near(panel))


def expand_kernel(ids_ref, panel_ref, right_ref, out_ref, mass_ref):
    for c in range(4):
        cols = pl.ds(c * TILE, TILE)
        total = jnp.zeros((2 * TILE, TILE), F32)
        for pair in range(KEEP // 2):
            lefts, rights = [], []
            for s in (2 * pair, 2 * pair + 1):
                k = ids_ref[s, c]
                inside = pl.ds(pl.multiple_of((k % 4) * TILE, TILE), TILE)
                parts = panel_ref[k // 4, pl.ds(2 * TILE, 8), inside].astype(jnp.int32).astype(F32)
                inverse = (16.0 / UNIT) / (parts[0:1] + parts[1:2] / UNIT)
                left = panel_ref[k // 4, pl.ds(0, 2 * TILE), inside].astype(jnp.int32).astype(F32)
                lefts.append((left * inverse).astype(BF16))
                rights.append(right_ref[pl.ds(8 * c, 8), s].reshape(TILE, TILE))
            total = total + jnp.dot(
                jnp.concatenate(lefts, axis=1),
                jnp.concatenate(rights, axis=0),
                preferred_element_type=F32,
            )
        total = total * total
        out_ref[:, cols] = total
        part = jnp.sum(total, axis=0, keepdims=True)
        for r in range(ROWS):
            mass_ref[r, :, cols] = part


def expand(ids, panel, right):
    return pl.pallas_call(
        expand_kernel,
        out_shape=(
            pltpu.VMEM((2 * TILE, 4 * TILE), F32),
            pltpu.VMEM((ROWS, 1, 4 * TILE), F32),
        ),
        in_specs=[SMEM] + [VMEM] * 2,
        out_specs=(VMEM, VMEM),
        compiler_params=pltpu.CompilerParams(vmem_limit_bytes=24 * 2**20),
        name="expand",
    )(ids, near(panel), near(right))


def scale_kernel(inflated_ref, mass_ref, flow_ref):
    mass = jnp.sum(mass_ref[...], axis=0)
    flow_ref[...] = inflated_ref[...] * (64.0 * TILE / mass)


def scale(inflated, mass):
    return pl.pallas_call(
        scale_kernel,
        out_shape=jax.ShapeDtypeStruct((2 * TILE, 4 * TILE), F32),
        in_specs=[VMEM, VMEM],
        out_specs=VMEM,
        name="scale",
    )(near(inflated), near(mass))


def on_device(weights, tile_mask):
    masked, sent = prepare(tile_mask, weights)
    got = exchange(sent, ROW)
    own = (lax.axis_index("y") // 2).reshape(1)
    placed, full = place(own, got, masked)
    right = exchange(placed, ROW)
    panel = lax.all_gather(full, ("z", "core"))
    there = (got[:, 44, :8].reshape(64, 4) > 0).astype(jnp.int32)
    rank = jnp.cumsum(there, axis=0) - there
    tile_ids = lax.broadcasted_iota(jnp.int32, (KEEP, 64, 4), 1)
    ranks = lax.broadcasted_iota(jnp.int32, (KEEP, 64, 4), 0)
    chosen = (there == 1)[None] & (rank[None] == ranks)
    ids = jnp.sum(jnp.where(chosen, tile_ids, 0), axis=1)
    inflated, mass = expand(ids, panel, right)
    return scale(inflated, exchange(mass, ROW))


def solution(mesh):
    split = Mesh(mesh.devices.reshape(NY, NX, NZ, NC), ("y", "x", "z", "core"))
    placed = P(ROW, ("z", "core"))
    return jax.shard_map(
        on_device, mesh=split, in_specs=(placed, placed), out_specs=placed, check_vma=False
    )
```

```python
import functools

import jax
import jax.numpy as jnp
from jax import lax
from jax.experimental import pallas as pl
from jax.experimental.pallas import tpu as pltpu
from jax.sharding import Mesh, PartitionSpec as P

KEEP = 8
TILE = 128
SLICE = 16
NY, NX, NZ, NC = 8, 4, 8, 2
ROWS = NY * NX
ROW = ("y", "x")
F32, BF16, I16 = jnp.float32, jnp.bfloat16, jnp.int16
UNIT = 16384.0
SLOTS = 9
HALF = TILE // 2
DEGREE = SLOTS * HALF
META = DEGREE + 8
PACKED = META + 8
COL = ("z", "core")
VMEM = pl.BlockSpec(memory_space=pltpu.VMEM)
SMEM = pl.BlockSpec(memory_space=pltpu.SMEM)


def exchange(blocks, axis):
    return lax.all_to_all(blocks, axis, split_axis=0, concat_axis=0, tiled=True)


def near(x):
    return pltpu.with_memory_space_constraint(x, pltpu.VMEM)


def split3(v):
    parts = []
    for _ in range(3):
        part = v.astype(BF16)
        parts.append(part)
        v = v - part.astype(F32)
    return parts


def prepare_kernel(mask_ref, w_ref, panel_ref, sent_ref):
    lane = lax.broadcasted_iota(jnp.int32, (1, TILE), 1)
    packed = jnp.zeros((1, TILE), F32)
    sums, masks = [], []
    for c in range(4):
        cols = pl.ds(c * TILE, TILE)
        total = jnp.zeros((1, TILE), F32)
        for t in range(2):
            on = mask_ref[t, c].astype(F32)
            masks.append(jnp.full((1, TILE), on, F32))
            packed = jnp.where(lane == t * 4 + c, on, packed)
            tile = w_ref[pl.ds(t * TILE, TILE), cols].astype(F32) * on
            total = total + jnp.sum(tile, axis=0, keepdims=True)
            panel_ref[pl.ds(t * TILE, TILE), cols] = (tile * UNIT).astype(jnp.int32).astype(I16)
            tile = tile.astype(BF16)
            for e in range(8):
                sent_ref[8 * c + e, pl.ds(t * SLICE, SLICE)] = tile[e * SLICE : (e + 1) * SLICE]
        rows = jnp.concatenate([*masks[2 * c : 2 * c + 2], jnp.zeros((6, TILE), F32)], axis=0)
        panel_ref[pl.ds(2 * TILE, 8), cols] = rows.astype(jnp.int32).astype(I16)
        sums.append(split3(total))
    rows = [sums[c][p].astype(F32) for p in range(3) for c in range(4)]
    for c in range(4):
        extra = jnp.concatenate([*rows, packed, packed, *masks[2 * c : 2 * c + 2]], axis=0).astype(BF16)
        for e in range(8):
            sent_ref[8 * c + e, pl.ds(2 * SLICE, SLICE)] = extra


def prepare(mask, weights):
    return pl.pallas_call(
        prepare_kernel,
        out_shape=(
            pltpu.VMEM((2 * TILE + 8, 4 * TILE), I16),
            pltpu.VMEM((ROWS, 3 * SLICE, TILE), BF16),
        ),
        in_specs=[SMEM, VMEM],
        out_specs=(VMEM,) * 2,
        name="prepare",
    )(mask, weights)


def pack_kernel(core_ref, panel_ref, other_ref, packed_ref):
    core = core_ref[0]
    lane = lax.broadcasted_iota(jnp.int32, (1, TILE), 1)

    def both(rows, q):
        cols = pl.ds((q % 4) * TILE, TILE)
        mine, other = panel_ref[rows, cols].astype(jnp.int32), other_ref[rows, cols].astype(jnp.int32)
        return jnp.where(core == q // 4, mine, other)

    count = jnp.zeros((1, TILE), jnp.int32)
    meta = jnp.zeros((1, TILE), jnp.int32)
    slots = []
    for t in range(2):
        for q in range(8):
            on = both(pl.ds(2 * TILE, 8), q)[t : t + 1]
            slot = jnp.where(on > 0, count, -1)
            count = count + on
            slots.append(slot)
            meta = jnp.where(lane == 8 * t + q, slot, meta)
    for s in range(SLOTS):
        kept = jnp.zeros((HALF, TILE), jnp.int32)
        for t in range(2):
            rows = pl.ds(pl.multiple_of(t * TILE + core * HALF, HALF), HALF)
            for q in range(8):
                kept = jnp.where(slots[8 * t + q] == s, both(rows, q), kept)
        packed_ref[pl.ds(s * HALF, HALF)] = kept.astype(I16)
    rows = jnp.concatenate([jnp.zeros((8, TILE), jnp.int32), meta, jnp.zeros((7, TILE), jnp.int32)], axis=0)
    packed_ref[pl.ds(DEGREE, 16)] = rows.astype(I16)


def pack(core, panel, other):
    return pl.pallas_call(
        pack_kernel,
        out_shape=pltpu.VMEM((PACKED, TILE), I16),
        in_specs=[SMEM, VMEM, VMEM],
        out_specs=VMEM,
        name="pack",
    )(core, near(panel), near(other))


def place_kernel(own_ref, got_ref, packed_ref, placed_ref, full_ref, slot_ref):
    total = jnp.zeros((SLICE, TILE), F32)
    masks, tiles = [], []
    for r in range(ROWS):
        extra = got_ref[r, pl.ds(2 * SLICE, SLICE)].astype(F32)
        total = total + extra
        tiles.append(extra[12:13])
        masks.append(extra[14:16])
    degree = total[0:4] + (total[4:8] + total[8:12])
    high = jnp.floor(degree * 16.0)
    low = (degree * 16.0 - high) * UNIT
    tiles = jnp.concatenate([*tiles, jnp.zeros((TILE - ROWS, TILE), F32)], axis=0).astype(BF16)
    counts = lax.dot_general(
        jnp.ones((8, TILE), BF16), tiles, (((1,), (1,)), ((), ())), preferred_element_type=F32
    )
    meta = packed_ref[pl.ds(META, 8)].astype(jnp.int32).astype(F32)
    rows = jnp.concatenate([high, low, meta[0:1], counts[0:7]], axis=0)
    full_ref[pl.ds(0, DEGREE)] = packed_ref[pl.ds(0, DEGREE)]
    full_ref[pl.ds(DEGREE, 16)] = rows.astype(jnp.int32).astype(I16)
    there = jnp.concatenate(masks, axis=0)
    above = lax.broadcasted_iota(jnp.int32, (64, 64), 0) > lax.broadcasted_iota(jnp.int32, (64, 64), 1)
    rank = jnp.dot(above.astype(BF16), there.astype(BF16), preferred_element_type=F32)
    slot_ref[...] = jnp.where(there > 0, rank, -1.0)
    own = own_ref[0]
    mine = jnp.zeros((1, TILE), F32)
    for c in range(4):
        mine = jnp.where(own == c, degree[c : c + 1], mine)
    kept = [jnp.zeros((SLICE, TILE), F32) for _ in range(KEEP)]
    for k in range(64):
        tile = got_ref[k // 2, pl.ds((k % 2) * SLICE, SLICE)].astype(F32)
        slot = jnp.broadcast_to(slot_ref[pl.ds(k, 1)], (SLICE, TILE))
        for s in range(KEEP):
            kept[s] = jnp.where(slot == s, tile, kept[s])
    for s in range(KEEP):
        tile = (kept[s] / mine).astype(BF16)
        for r in range(ROWS):
            placed_ref[r, s] = tile


def place(own, got, packed):
    return pl.pallas_call(
        place_kernel,
        out_shape=(
            pltpu.VMEM((ROWS, KEEP, SLICE, TILE), BF16),
            pltpu.VMEM((PACKED, TILE), I16),
        ),
        in_specs=[SMEM, VMEM, VMEM],
        out_specs=(VMEM, VMEM),
        scratch_shapes=[pltpu.VMEM((64, TILE), F32)],
        name="place",
    )(own, near(got), near(packed))


def expand_kernel(dense, ids_ref, slots_ref, full_ref, *refs):
    panel_ref = refs[0] if dense else None
    right_ref, out_ref, mass_ref, inverse_ref = refs[-4:]
    for col in range(NZ * NC):
        parts = full_ref[col, pl.ds(DEGREE, 8)].astype(jnp.int32).astype(F32)
        inverse_ref[col] = (16.0 / UNIT) / (parts[0:4] + parts[4:8] / UNIT)
    for c in range(4):
        cols = pl.ds(c * TILE, TILE)
        total = jnp.zeros((2 * TILE, TILE), F32)
        for pair in range(KEEP // 2):
            lefts, rights = [], []
            for s in (2 * pair, 2 * pair + 1):
                k = ids_ref[s, c]
                inverse = inverse_ref[k // 4, pl.ds(k % 4, 1), :]
                if dense:
                    inside = pl.ds(pl.multiple_of((k % 4) * TILE, TILE), TILE)
                    left = panel_ref[k // 4, pl.ds(0, 2 * TILE), inside].astype(jnp.int32).astype(F32)
                    lefts.append((left * inverse).astype(BF16))
                else:
                    parts = []
                    for t in range(2):
                        slot = slots_ref[k // 8, 8 * t + k % 8]
                        start = pl.multiple_of(jnp.maximum(slot, 0) * HALF, HALF)
                        scaled = jnp.where(slot >= 0, inverse, 0.0)
                        for core in range(NC):
                            part = full_ref[(k // 8) * NC + core, pl.ds(start, HALF)].astype(jnp.int32)
                            parts.append((part.astype(F32) * scaled).astype(BF16))
                    lefts.append(jnp.concatenate(parts, axis=0))
                rights.append(right_ref[pl.ds(8 * c, 8), s].reshape(TILE, TILE))
            total = total + jnp.dot(
                jnp.concatenate(lefts, axis=1),
                jnp.concatenate(rights, axis=0),
                preferred_element_type=F32,
            )
        total = total * total
        out_ref[:, cols] = total
        part = jnp.sum(total, axis=0, keepdims=True)
        for r in range(ROWS):
            mass_ref[r, :, cols] = part


def expand(ids, slots, full, *panels_and_right):
    dense = len(panels_and_right) == 2
    return pl.pallas_call(
        functools.partial(expand_kernel, dense),
        out_shape=(
            pltpu.VMEM((2 * TILE, 4 * TILE), F32),
            pltpu.VMEM((ROWS, 1, 4 * TILE), F32),
        ),
        in_specs=[SMEM, SMEM] + [VMEM] * (1 + len(panels_and_right)),
        out_specs=(VMEM, VMEM),
        scratch_shapes=[pltpu.VMEM((NZ * NC, 4, TILE), F32)],
        compiler_params=pltpu.CompilerParams(vmem_limit_bytes=24 * 2**20),
        name="expand_dense" if dense else "expand",
    )(ids, slots, full, *panels_and_right)


def scale_kernel(inflated_ref, mass_ref, flow_ref):
    mass = jnp.sum(mass_ref[...], axis=0)
    flow_ref[...] = inflated_ref[...] * (64.0 * TILE / mass)


def scale(inflated, mass):
    return pl.pallas_call(
        scale_kernel,
        out_shape=jax.ShapeDtypeStruct((2 * TILE, 4 * TILE), F32),
        in_specs=[VMEM, VMEM],
        out_specs=VMEM,
        name="scale",
    )(near(inflated), near(mass))


def on_device(weights, tile_mask):
    panel, sent = prepare(tile_mask, weights)
    got = exchange(sent, ROW)
    other = lax.ppermute(panel, "core", [(0, 1), (1, 0)])
    packed = pack(lax.axis_index("core").reshape(1), panel, other)
    own = (lax.axis_index("y") // 2).reshape(1)
    placed, full = place(own, got, packed)
    right = exchange(placed, ROW)
    full = lax.all_gather(full, COL)
    there = (got[:, 44, :8].reshape(64, 4) > 0).astype(jnp.int32)
    rank = jnp.cumsum(there, axis=0) - there
    tile_ids = lax.broadcasted_iota(jnp.int32, (KEEP, 64, 4), 1)
    ranks = lax.broadcasted_iota(jnp.int32, (KEEP, 64, 4), 0)
    chosen = (there == 1)[None] & (rank[None] == ranks)
    ids = jnp.sum(jnp.where(chosen, tile_ids, 0), axis=1)
    slots = full[::2, META, :16].astype(jnp.int32)
    counts = full[:, META + 1, :ROWS].astype(jnp.int32).reshape(NZ, NC, ROWS).sum(axis=1)

    def overfull():
        return expand(ids, slots, full, lax.all_gather(panel, COL), right)

    def fits():
        return expand(ids, slots, full, right)

    inflated, mass = lax.cond(jnp.max(counts) > SLOTS, overfull, fits)
    return scale(inflated, exchange(mass, ROW))


def solution(mesh):
    split = Mesh(mesh.devices.reshape(NY, NX, NZ, NC), ("y", "x", "z", "core"))
    placed = P(ROW, ("z", "core"))
    return jax.shard_map(
        on_device, mesh=split, in_specs=(placed, placed), out_specs=placed, check_vma=False
    )
```

```python
import functools

import jax
import jax.numpy as jnp
from jax import lax
from jax.experimental import pallas as pl
from jax.experimental.pallas import tpu as pltpu
from jax.sharding import Mesh, PartitionSpec as P

KEEP = 8
TILE = 128
SLICE = 16
NY, NX, NZ, NC = 8, 4, 8, 2
ROWS = NY * NX
ROW = ("y", "x")
F32, BF16, I16 = jnp.float32, jnp.bfloat16, jnp.int16
UNIT = 16384.0
SLOTS = 9
HALF = TILE // 2
DEGREE = SLOTS * HALF
META = DEGREE + 8
PACKED = META + 8
COL = ("z", "core")
VMEM = pl.BlockSpec(memory_space=pltpu.VMEM)
SMEM = pl.BlockSpec(memory_space=pltpu.SMEM)


def exchange(blocks, axis):
    return lax.all_to_all(blocks, axis, split_axis=0, concat_axis=0, tiled=True)


def near(x):
    return pltpu.with_memory_space_constraint(x, pltpu.VMEM)


def split3(v):
    parts = []
    for _ in range(3):
        part = v.astype(BF16)
        parts.append(part)
        v = v - part.astype(F32)
    return parts


def slice_kernel(mask_ref, w_ref, sent_ref):
    lane = lax.broadcasted_iota(jnp.int32, (1, TILE), 1)
    packed = jnp.zeros((1, TILE), F32)
    sums, masks = [], []
    for c in range(4):
        total = jnp.zeros((1, TILE), F32)
        for t in range(2):
            on = mask_ref[t, c].astype(F32)
            masks.append(jnp.full((1, TILE), on, F32))
            packed = jnp.where(lane == t * 4 + c, on, packed)
            tile = w_ref[pl.ds(t * TILE, TILE), pl.ds(c * TILE, TILE)].astype(F32) * on
            total = total + jnp.sum(tile, axis=0, keepdims=True)
            tile = tile.astype(BF16)
            for e in range(8):
                sent_ref[8 * c + e, pl.ds(t * SLICE, SLICE)] = tile[e * SLICE : (e + 1) * SLICE]
        sums.append(split3(total))
    rows = [sums[c][p].astype(F32) for p in range(3) for c in range(4)]
    for c in range(4):
        extra = jnp.concatenate([*rows, packed, packed, *masks[2 * c : 2 * c + 2]], axis=0).astype(BF16)
        for e in range(8):
            sent_ref[8 * c + e, pl.ds(2 * SLICE, SLICE)] = extra


def slices(mask, weights):
    return pl.pallas_call(
        slice_kernel,
        out_shape=jax.ShapeDtypeStruct((ROWS, 3 * SLICE, TILE), BF16),
        in_specs=[SMEM, VMEM],
        out_specs=VMEM,
        name="slices",
    )(mask, weights)


def panel_kernel(mask_ref, w_ref, panel_ref):
    for c in range(4):
        cols = pl.ds(c * TILE, TILE)
        masks = []
        for t in range(2):
            on = mask_ref[t, c].astype(F32)
            masks.append(jnp.full((1, TILE), on, F32))
            tile = w_ref[pl.ds(t * TILE, TILE), cols].astype(F32) * (on * UNIT)
            panel_ref[pl.ds(t * TILE, TILE), cols] = tile.astype(jnp.int32).astype(I16)
        rows = jnp.concatenate([*masks, jnp.zeros((6, TILE), F32)], axis=0)
        panel_ref[pl.ds(2 * TILE, 8), cols] = rows.astype(jnp.int32).astype(I16)


def fixed_panel(mask, weights):
    return pl.pallas_call(
        panel_kernel,
        out_shape=pltpu.VMEM((2 * TILE + 8, 4 * TILE), I16),
        in_specs=[SMEM, VMEM],
        out_specs=VMEM,
        name="panel",
    )(mask, weights)


def pack_kernel(core_ref, panel_ref, other_ref, packed_ref):
    core = core_ref[0]
    lane = lax.broadcasted_iota(jnp.int32, (1, TILE), 1)

    def both(rows, q):
        cols = pl.ds((q % 4) * TILE, TILE)
        mine, other = panel_ref[rows, cols].astype(jnp.int32), other_ref[rows, cols].astype(jnp.int32)
        return jnp.where(core == q // 4, mine, other)

    count = jnp.zeros((1, TILE), jnp.int32)
    meta = jnp.zeros((1, TILE), jnp.int32)
    slots = []
    for t in range(2):
        for q in range(8):
            on = both(pl.ds(2 * TILE, 8), q)[t : t + 1]
            slot = jnp.where(on > 0, count, -1)
            count = count + on
            slots.append(slot)
            meta = jnp.where(lane == 8 * t + q, slot, meta)
    for s in range(SLOTS):
        kept = jnp.zeros((HALF, TILE), jnp.int32)
        for t in range(2):
            rows = pl.ds(pl.multiple_of(t * TILE + core * HALF, HALF), HALF)
            for q in range(8):
                kept = jnp.where(slots[8 * t + q] == s, both(rows, q), kept)
        packed_ref[pl.ds(s * HALF, HALF)] = kept.astype(I16)
    rows = jnp.concatenate([jnp.zeros((8, TILE), jnp.int32), meta, jnp.zeros((7, TILE), jnp.int32)], axis=0)
    packed_ref[pl.ds(DEGREE, 16)] = rows.astype(I16)


def pack(core, panel, other):
    return pl.pallas_call(
        pack_kernel,
        out_shape=pltpu.VMEM((PACKED, TILE), I16),
        in_specs=[SMEM, VMEM, VMEM],
        out_specs=VMEM,
        name="pack",
    )(core, near(panel), near(other))


def place_kernel(own_ref, got_ref, packed_ref, placed_ref, full_ref, ids_ref, slot_ref):
    total = jnp.zeros((SLICE, TILE), F32)
    masks, tiles = [], []
    for r in range(ROWS):
        extra = got_ref[r, pl.ds(2 * SLICE, SLICE)].astype(F32)
        total = total + extra
        tiles.append(extra[12:13])
        masks.append(extra[14:16])
    degree = total[0:4] + (total[4:8] + total[8:12])
    high = jnp.floor(degree * 16.0)
    low = (degree * 16.0 - high) * UNIT
    tiles = jnp.concatenate(tiles, axis=0)
    row = lax.broadcasted_iota(jnp.int32, (ROWS, TILE), 0)
    lower = lax.broadcasted_iota(jnp.int32, (ROWS, TILE), 1) // 4
    pair = tiles + jnp.where(lower == 0, pltpu.roll(tiles, TILE - 4, 1), pltpu.roll(tiles, 4, 1))
    above = lax.broadcasted_iota(jnp.int32, (ROWS, ROWS), 0) > lax.broadcasted_iota(jnp.int32, (ROWS, ROWS), 1)
    rank = jnp.dot(above.astype(BF16), pair.astype(BF16), preferred_element_type=F32)
    rank = rank + jnp.where(lower == 1, pltpu.roll(tiles, 4, 1), 0.0)
    kept_row = (2 * row + lower).astype(F32)
    for s in range(KEEP):
        hit = jnp.where((tiles > 0) & (rank == s) & (lower < 2), kept_row, 0.0)
        hit = jnp.sum(hit, axis=0, keepdims=True)
        ids_ref[pl.ds(s, 1)] = (hit + pltpu.roll(hit, TILE - 4, 1)).astype(jnp.int32)
    tiles = jnp.concatenate([tiles, jnp.zeros((TILE - ROWS, TILE), F32)], axis=0).astype(BF16)
    counts = lax.dot_general(
        jnp.ones((8, TILE), BF16), tiles, (((1,), (1,)), ((), ())), preferred_element_type=F32
    )
    meta = packed_ref[pl.ds(META, 8)].astype(jnp.int32).astype(F32)
    rows = jnp.concatenate([high, low, meta[0:1], counts[0:7]], axis=0)
    full_ref[pl.ds(0, DEGREE)] = packed_ref[pl.ds(0, DEGREE)]
    full_ref[pl.ds(DEGREE, 16)] = rows.astype(jnp.int32).astype(I16)
    there = jnp.concatenate(masks, axis=0)
    above = lax.broadcasted_iota(jnp.int32, (64, 64), 0) > lax.broadcasted_iota(jnp.int32, (64, 64), 1)
    rank = jnp.dot(above.astype(BF16), there.astype(BF16), preferred_element_type=F32)
    slot_ref[...] = jnp.where(there > 0, rank, -1.0)
    own = own_ref[0]
    mine = jnp.zeros((1, TILE), F32)
    for c in range(4):
        mine = jnp.where(own == c, degree[c : c + 1], mine)
    kept = [jnp.zeros((SLICE, TILE), F32) for _ in range(KEEP)]
    for k in range(64):
        tile = got_ref[k // 2, pl.ds((k % 2) * SLICE, SLICE)].astype(F32)
        slot = jnp.broadcast_to(slot_ref[pl.ds(k, 1)], (SLICE, TILE))
        for s in range(KEEP):
            kept[s] = jnp.where(slot == s, tile, kept[s])
    for s in range(KEEP):
        tile = (kept[s] / mine).astype(BF16)
        for r in range(ROWS):
            placed_ref[r, s] = tile


def place(own, got, packed):
    return pl.pallas_call(
        place_kernel,
        out_shape=(
            pltpu.VMEM((ROWS, KEEP, SLICE, TILE), BF16),
            pltpu.VMEM((PACKED, TILE), I16),
            jax.ShapeDtypeStruct((KEEP, TILE), jnp.int32),
        ),
        in_specs=[SMEM, VMEM, VMEM],
        out_specs=(VMEM, VMEM, VMEM),
        scratch_shapes=[pltpu.VMEM((64, TILE), F32)],
        name="place",
    )(own, near(got), near(packed))


def expand_kernel(dense, ids_ref, slots_ref, full_ref, *refs):
    panel_ref = refs[0] if dense else None
    right_ref, out_ref, mass_ref, inverse_ref = refs[-4:]
    for col in range(NZ * NC):
        parts = full_ref[col, pl.ds(DEGREE, 8)].astype(jnp.int32).astype(F32)
        inverse_ref[col] = (16.0 / UNIT) / (parts[0:4] + parts[4:8] / UNIT)
    for c in range(4):
        cols = pl.ds(c * TILE, TILE)
        total = jnp.zeros((2 * TILE, TILE), F32)
        for pair in range(KEEP // 2):
            lefts, rights = [], []
            for s in (2 * pair, 2 * pair + 1):
                k = ids_ref[s, c]
                inverse = inverse_ref[k // 4, pl.ds(k % 4, 1), :]
                if dense:
                    inside = pl.ds(pl.multiple_of((k % 4) * TILE, TILE), TILE)
                    left = panel_ref[k // 4, pl.ds(0, 2 * TILE), inside].astype(jnp.int32).astype(F32)
                    lefts.append((left * inverse).astype(BF16))
                else:
                    parts = []
                    for t in range(2):
                        slot = slots_ref[k // 8, 8 * t + k % 8]
                        start = pl.multiple_of(jnp.maximum(slot, 0) * HALF, HALF)
                        scaled = jnp.where(slot >= 0, inverse, 0.0)
                        for core in range(NC):
                            part = full_ref[(k // 8) * NC + core, pl.ds(start, HALF)].astype(jnp.int32)
                            parts.append((part.astype(F32) * scaled).astype(BF16))
                    lefts.append(jnp.concatenate(parts, axis=0))
                rights.append(right_ref[pl.ds(8 * c, 8), s].reshape(TILE, TILE))
            total = total + jnp.dot(
                jnp.concatenate(lefts, axis=1),
                jnp.concatenate(rights, axis=0),
                preferred_element_type=F32,
            )
        total = total * total
        out_ref[:, cols] = total
        part = jnp.sum(total, axis=0, keepdims=True)
        for r in range(ROWS):
            mass_ref[r, :, cols] = part


def expand(ids, slots, full, *panels_and_right):
    dense = len(panels_and_right) == 2
    return pl.pallas_call(
        functools.partial(expand_kernel, dense),
        out_shape=(
            pltpu.VMEM((2 * TILE, 4 * TILE), F32),
            pltpu.VMEM((ROWS, 1, 4 * TILE), F32),
        ),
        in_specs=[SMEM, SMEM] + [VMEM] * (1 + len(panels_and_right)),
        out_specs=(VMEM, VMEM),
        scratch_shapes=[pltpu.VMEM((NZ * NC, 4, TILE), F32)],
        compiler_params=pltpu.CompilerParams(vmem_limit_bytes=24 * 2**20),
        name="expand_dense" if dense else "expand",
    )(ids, slots, full, *panels_and_right)


def scale_kernel(inflated_ref, mass_ref, flow_ref):
    mass = jnp.sum(mass_ref[...], axis=0)
    flow_ref[...] = inflated_ref[...] * (64.0 * TILE / mass)


def scale(inflated, mass):
    return pl.pallas_call(
        scale_kernel,
        out_shape=pltpu.HBM((2 * TILE, 4 * TILE), F32),
        in_specs=[VMEM, VMEM],
        out_specs=VMEM,
        name="scale",
    )(near(inflated), near(mass))


def on_device(weights, tile_mask):
    got = exchange(slices(tile_mask, weights), ROW)
    panel = fixed_panel(tile_mask, weights)
    other = lax.ppermute(panel, "core", [(0, 1), (1, 0)])
    packed = pack(lax.axis_index("core").reshape(1), panel, other)
    own = (lax.axis_index("y") // 2).reshape(1)
    placed, full, ids = place(own, got, packed)
    right = exchange(placed, ROW)
    full = lax.all_gather(full, COL)
    slots = full[::2, META, :16].astype(jnp.int32)
    inflated, mass = expand(ids, slots, full, right)
    mass = exchange(mass, ROW)
    counts = full[:, META + 1, :ROWS].astype(jnp.int32).reshape(NZ, NC, ROWS).sum(axis=1)

    def overfull():
        inflated, mass = expand(ids, slots, full, lax.all_gather(panel, COL), right)
        return scale(inflated, exchange(mass, ROW))

    def fits():
        return scale(inflated, mass)

    return lax.cond(jnp.max(counts) > SLOTS, overfull, fits)


def solution(mesh):
    split = Mesh(mesh.devices.reshape(NY, NX, NZ, NC), ("y", "x", "z", "core"))
    placed = P(ROW, ("z", "core"))
    return jax.shard_map(
        on_device, mesh=split, in_specs=(placed, placed), out_specs=placed, check_vma=False
    )
```

```python
import functools

import jax
import jax.numpy as jnp
from jax import lax
from jax.experimental import pallas as pl
from jax.experimental.pallas import tpu as pltpu
from jax.sharding import Mesh, PartitionSpec as P

KEEP = 8
TILE = 128
SLICE = 16
NY, NX, NZ, NC = 8, 4, 8, 2
ROWS = NY * NX
ROW = ("y", "x")
F32, BF16, I16 = jnp.float32, jnp.bfloat16, jnp.int16
UNIT = 16384.0
SLOTS = 9
HALF = TILE // 2
DEGREE = SLOTS * HALF
META = DEGREE + 8
PACKED = META + 8
COL = ("z", "core")
LIMIT = pltpu.CompilerParams(vmem_limit_bytes=24 * 2**20)
VMEM = pl.BlockSpec(memory_space=pltpu.VMEM)
SMEM = pl.BlockSpec(memory_space=pltpu.SMEM)


def exchange(blocks, axis):
    return lax.all_to_all(blocks, axis, split_axis=0, concat_axis=0, tiled=True)


def near(x):
    return pltpu.with_memory_space_constraint(x, pltpu.VMEM)


def split3(v):
    parts = []
    for _ in range(3):
        part = v.astype(BF16)
        parts.append(part)
        v = v - part.astype(F32)
    return parts


def slice_kernel(mask_ref, w_ref, sent_ref):
    lane = lax.broadcasted_iota(jnp.int32, (1, TILE), 1)
    packed = jnp.zeros((1, TILE), F32)
    sums, masks = [], []
    for c in range(4):
        total = jnp.zeros((1, TILE), F32)
        for t in range(2):
            on = mask_ref[t, c].astype(F32)
            masks.append(jnp.full((1, TILE), on, F32))
            packed = jnp.where(lane == t * 4 + c, on, packed)
            tile = w_ref[pl.ds(t * TILE, TILE), pl.ds(c * TILE, TILE)].astype(F32) * on
            total = total + jnp.sum(tile, axis=0, keepdims=True)
            tile = tile.astype(BF16)
            for e in range(8):
                sent_ref[8 * c + e, pl.ds(t * SLICE, SLICE)] = tile[e * SLICE : (e + 1) * SLICE]
        sums.append(split3(total))
    rows = [sums[c][p].astype(F32) for p in range(3) for c in range(4)]
    for c in range(4):
        extra = jnp.concatenate([*rows, packed, packed, *masks[2 * c : 2 * c + 2]], axis=0).astype(BF16)
        for e in range(8):
            sent_ref[8 * c + e, pl.ds(2 * SLICE, SLICE)] = extra


def slices(mask, weights):
    return pl.pallas_call(
        slice_kernel,
        out_shape=jax.ShapeDtypeStruct((ROWS, 3 * SLICE, TILE), BF16),
        in_specs=[SMEM, VMEM],
        out_specs=VMEM,
        name="slices",
    )(mask, weights)


def panel_kernel(mask_ref, w_ref, panel_ref):
    for c in range(4):
        cols = pl.ds(c * TILE, TILE)
        masks = []
        for t in range(2):
            on = mask_ref[t, c].astype(F32)
            masks.append(jnp.full((1, TILE), on, F32))
            tile = w_ref[pl.ds(t * TILE, TILE), cols].astype(F32) * (on * UNIT)
            panel_ref[pl.ds(t * TILE, TILE), cols] = tile.astype(jnp.int32).astype(I16)
        rows = jnp.concatenate([*masks, jnp.zeros((6, TILE), F32)], axis=0)
        panel_ref[pl.ds(2 * TILE, 8), cols] = rows.astype(jnp.int32).astype(I16)


def fixed_panel(mask, weights):
    return pl.pallas_call(
        panel_kernel,
        out_shape=pltpu.VMEM((2 * TILE + 8, 4 * TILE), I16),
        in_specs=[SMEM, VMEM],
        out_specs=VMEM,
        name="panel",
    )(mask, weights)


def pack_kernel(core_ref, panel_ref, other_ref, packed_ref):
    core = core_ref[0]
    lane = lax.broadcasted_iota(jnp.int32, (1, TILE), 1)

    def both(rows, q):
        cols = pl.ds((q % 4) * TILE, TILE)
        mine, other = panel_ref[rows, cols].astype(jnp.int32), other_ref[rows, cols].astype(jnp.int32)
        return jnp.where(core == q // 4, mine, other)

    count = jnp.zeros((1, TILE), jnp.int32)
    meta = jnp.zeros((1, TILE), jnp.int32)
    slots = []
    for t in range(2):
        for q in range(8):
            on = both(pl.ds(2 * TILE, 8), q)[t : t + 1]
            slot = jnp.where(on > 0, count, -1)
            count = count + on
            slots.append(slot)
            meta = jnp.where(lane == 8 * t + q, slot, meta)
    for s in range(SLOTS):
        kept = jnp.zeros((HALF, TILE), jnp.int32)
        for t in range(2):
            rows = pl.ds(pl.multiple_of(t * TILE + core * HALF, HALF), HALF)
            for q in range(8):
                kept = jnp.where(slots[8 * t + q] == s, both(rows, q), kept)
        packed_ref[pl.ds(s * HALF, HALF)] = kept.astype(I16)
    rows = jnp.concatenate([jnp.zeros((8, TILE), jnp.int32), meta, jnp.zeros((7, TILE), jnp.int32)], axis=0)
    packed_ref[pl.ds(DEGREE, 16)] = rows.astype(I16)


def pack(core, panel, other):
    return pl.pallas_call(
        pack_kernel,
        out_shape=pltpu.VMEM((PACKED, TILE), I16),
        in_specs=[SMEM, VMEM, VMEM],
        out_specs=VMEM,
        name="pack",
    )(core, near(panel), near(other))


def place_kernel(own_ref, got_ref, packed_ref, placed_ref, full_ref, ids_ref, slot_ref):
    total = jnp.zeros((SLICE, TILE), F32)
    masks, tiles = [], []
    for r in range(ROWS):
        extra = got_ref[r, pl.ds(2 * SLICE, SLICE)].astype(F32)
        total = total + extra
        tiles.append(extra[12:13])
        masks.append(extra[14:16])
    degree = total[0:4] + (total[4:8] + total[8:12])
    high = jnp.floor(degree * 16.0)
    low = (degree * 16.0 - high) * UNIT
    tiles = jnp.concatenate(tiles, axis=0)
    row = lax.broadcasted_iota(jnp.int32, (ROWS, TILE), 0)
    lower = lax.broadcasted_iota(jnp.int32, (ROWS, TILE), 1) // 4
    pair = tiles + jnp.where(lower == 0, pltpu.roll(tiles, TILE - 4, 1), pltpu.roll(tiles, 4, 1))
    above = lax.broadcasted_iota(jnp.int32, (ROWS, ROWS), 0) > lax.broadcasted_iota(jnp.int32, (ROWS, ROWS), 1)
    rank = jnp.dot(above.astype(BF16), pair.astype(BF16), preferred_element_type=F32)
    rank = rank + jnp.where(lower == 1, pltpu.roll(tiles, 4, 1), 0.0)
    kept_row = (2 * row + lower).astype(F32)
    for s in range(KEEP):
        hit = jnp.where((tiles > 0) & (rank == s) & (lower < 2), kept_row, 0.0)
        hit = jnp.sum(hit, axis=0, keepdims=True)
        ids_ref[pl.ds(s, 1)] = (hit + pltpu.roll(hit, TILE - 4, 1)).astype(jnp.int32)
    tiles = jnp.concatenate([tiles, jnp.zeros((TILE - ROWS, TILE), F32)], axis=0).astype(BF16)
    counts = lax.dot_general(
        jnp.ones((8, TILE), BF16), tiles, (((1,), (1,)), ((), ())), preferred_element_type=F32
    )
    meta = packed_ref[pl.ds(META, 8)].astype(jnp.int32).astype(F32)
    rows = jnp.concatenate([high, low, meta[0:1], counts[0:7]], axis=0)
    full_ref[pl.ds(0, DEGREE)] = packed_ref[pl.ds(0, DEGREE)]
    full_ref[pl.ds(DEGREE, 16)] = rows.astype(jnp.int32).astype(I16)
    there = jnp.concatenate(masks, axis=0)
    above = lax.broadcasted_iota(jnp.int32, (64, 64), 0) > lax.broadcasted_iota(jnp.int32, (64, 64), 1)
    rank = jnp.dot(above.astype(BF16), there.astype(BF16), preferred_element_type=F32)
    slot_ref[...] = jnp.where(there > 0, rank, -1.0)
    own = own_ref[0]
    mine = jnp.zeros((1, TILE), F32)
    for c in range(4):
        mine = jnp.where(own == c, degree[c : c + 1], mine)
    kept = [jnp.zeros((SLICE, TILE), F32) for _ in range(KEEP)]
    for k in range(64):
        tile = got_ref[k // 2, pl.ds((k % 2) * SLICE, SLICE)].astype(F32)
        slot = jnp.broadcast_to(slot_ref[pl.ds(k, 1)], (SLICE, TILE))
        for s in range(KEEP):
            kept[s] = jnp.where(slot == s, tile, kept[s])
    for s in range(KEEP):
        tile = (kept[s] / mine).astype(BF16)
        for r in range(ROWS):
            placed_ref[r, s] = tile


def place(own, got, packed):
    return pl.pallas_call(
        place_kernel,
        out_shape=(
            pltpu.VMEM((ROWS, KEEP, SLICE, TILE), BF16),
            pltpu.VMEM((PACKED, TILE), I16),
            jax.ShapeDtypeStruct((KEEP, TILE), jnp.int32),
        ),
        in_specs=[SMEM, VMEM, VMEM],
        out_specs=(VMEM, VMEM, VMEM),
        scratch_shapes=[pltpu.VMEM((64, TILE), F32)],
        name="place",
    )(own, near(got), near(packed))


def expand_kernel(dense, ids_ref, slots_ref, full_ref, *refs):
    panel_ref = refs[0] if dense else None
    right_ref, out_ref, mass_ref, most_ref, inverse_ref = refs[-5:]
    most = jnp.zeros((8, TILE), jnp.int32)
    for z in range(NZ):
        held = jnp.zeros((8, TILE), jnp.int32)
        for col in range(NC * z, NC * z + NC):
            rows = full_ref[col, pl.ds(DEGREE, 16)].astype(jnp.int32)
            parts = rows[0:8].astype(F32)
            inverse_ref[col] = (16.0 / UNIT) / (parts[0:4] + parts[4:8] / UNIT)
            held = held + rows[8:16]
        most = jnp.maximum(most, held)
    most_ref[0] = jnp.max(most[1:2, :ROWS])
    for c in range(4):
        cols = pl.ds(c * TILE, TILE)
        total = jnp.zeros((2 * TILE, TILE), F32)
        for pair in range(KEEP // 2):
            lefts, rights = [], []
            for s in (2 * pair, 2 * pair + 1):
                k = ids_ref[s, c]
                inverse = inverse_ref[k // 4, pl.ds(k % 4, 1), :]
                if dense:
                    inside = pl.ds(pl.multiple_of((k % 4) * TILE, TILE), TILE)
                    left = panel_ref[k // 4, pl.ds(0, 2 * TILE), inside].astype(jnp.int32).astype(F32)
                    lefts.append((left * inverse).astype(BF16))
                else:
                    parts = []
                    for t in range(2):
                        slot = slots_ref[k // 8, 8 * t + k % 8]
                        start = pl.multiple_of(jnp.maximum(slot, 0) * HALF, HALF)
                        scaled = jnp.where(slot >= 0, inverse, 0.0)
                        for core in range(NC):
                            part = full_ref[(k // 8) * NC + core, pl.ds(start, HALF)].astype(jnp.int32)
                            parts.append((part.astype(F32) * scaled).astype(BF16))
                    lefts.append(jnp.concatenate(parts, axis=0))
                rights.append(right_ref[pl.ds(8 * c, 8), s].reshape(TILE, TILE))
            total = total + jnp.dot(
                jnp.concatenate(lefts, axis=1),
                jnp.concatenate(rights, axis=0),
                preferred_element_type=F32,
            )
        total = total * total
        out_ref[:, cols] = total
        part = jnp.sum(total, axis=0, keepdims=True)
        for r in range(ROWS):
            mass_ref[r, :, cols] = part


def expand(ids, slots, full, *panels_and_right):
    dense = len(panels_and_right) == 2
    return pl.pallas_call(
        functools.partial(expand_kernel, dense),
        out_shape=(
            pltpu.VMEM((2 * TILE, 4 * TILE), F32),
            jax.ShapeDtypeStruct((ROWS, 1, 4 * TILE), F32),
            jax.ShapeDtypeStruct((1,), jnp.int32),
        ),
        in_specs=[SMEM, SMEM] + [VMEM] * (1 + len(panels_and_right)),
        out_specs=(VMEM, VMEM, SMEM),
        scratch_shapes=[pltpu.VMEM((NZ * NC, 4, TILE), F32)],
        compiler_params=LIMIT,
        name="expand_dense" if dense else "expand",
    )(ids, slots, full, *panels_and_right)


def scale_kernel(inflated_ref, mass_ref, flow_ref):
    mass = jnp.sum(mass_ref[...], axis=0)
    flow_ref[...] = inflated_ref[...] * (64.0 * TILE / mass)


def scale(inflated, mass):
    return pl.pallas_call(
        scale_kernel,
        out_shape=pltpu.HBM((2 * TILE, 4 * TILE), F32),
        in_specs=[VMEM, VMEM],
        out_specs=VMEM,
        name="scale",
    )(near(inflated), near(mass))


def on_device(weights, tile_mask):
    got = exchange(slices(tile_mask, weights), ROW)
    panel = fixed_panel(tile_mask, weights)
    other = lax.ppermute(panel, "core", [(0, 1), (1, 0)])
    packed = pack(lax.axis_index("core").reshape(1), panel, other)
    own = (lax.axis_index("y") // 2).reshape(1)
    placed, full, ids = place(own, got, packed)
    right = exchange(placed, ROW)
    full = lax.all_gather(full, COL)
    slots = full[::2, META, :16].astype(jnp.int32)
    inflated, mass, most = expand(ids, slots, full, right)
    mass = exchange(mass, ROW)

    def overfull():
        inflated, mass, _ = expand(ids, slots, full, lax.all_gather(panel, COL), right)
        return scale(inflated, exchange(mass, ROW))

    return lax.cond(most[0] > SLOTS, overfull, lambda: scale(inflated, mass))


def solution(mesh):
    split = Mesh(mesh.devices.reshape(NY, NX, NZ, NC), ("y", "x", "z", "core"))
    placed = P(ROW, ("z", "core"))
    return jax.shard_map(
        on_device, mesh=split, in_specs=(placed, placed), out_specs=placed, check_vma=False
    )
```

```python
import functools

import jax
import jax.numpy as jnp
from jax import lax
from jax.experimental import pallas as pl
from jax.experimental.pallas import tpu as pltpu
from jax.sharding import Mesh, PartitionSpec as P

KEEP = 8
TILE = 128
SLICE = 16
NY, NX, NZ, NC = 8, 4, 8, 2
ROWS = NY * NX
FIRST = ((4, 2), (0, 0), (4, 2))
F32, BF16, I16 = jnp.float32, jnp.bfloat16, jnp.int16
UNIT = 16384.0
SLOTS = 9
HALF = TILE // 2
DEGREE = SLOTS * HALF
META = DEGREE + 8
PACKED = META + 8
COL = ("z", "core")
LIMIT = pltpu.CompilerParams(vmem_limit_bytes=24 * 2**20)
VMEM = pl.BlockSpec(memory_space=pltpu.VMEM)
SMEM = pl.BlockSpec(memory_space=pltpu.SMEM)


def row_at(place, first):
    return (place // NX + first[0]) % NY * NX + (place + first[1]) % NX


def place_of(row, first):
    return row_at(row, (-first[0], -first[1]))


def exchange(blocks, first):
    group = [row_at(place, first) for place in range(ROWS)]
    return lax.all_to_all(
        blocks, "row", split_axis=0, concat_axis=0, tiled=True, axis_index_groups=[group]
    )


def near(x):
    return pltpu.with_memory_space_constraint(x, pltpu.VMEM)


def split3(v):
    parts = []
    for _ in range(3):
        part = v.astype(BF16)
        parts.append(part)
        v = v - part.astype(F32)
    return parts


def slice_kernel(mask_ref, w_ref, sent_ref):
    lane = lax.broadcasted_iota(jnp.int32, (1, TILE), 1)
    packed = jnp.zeros((1, TILE), F32)
    sums, masks = [], []
    for c in range(4):
        total = jnp.zeros((1, TILE), F32)
        for t in range(2):
            on = mask_ref[t, c].astype(F32)
            masks.append(jnp.full((1, TILE), on, F32))
            packed = jnp.where(lane == t * 4 + c, on, packed)
            tile = w_ref[pl.ds(t * TILE, TILE), pl.ds(c * TILE, TILE)].astype(F32) * on
            total = total + jnp.sum(tile, axis=0, keepdims=True)
            tile = tile.astype(BF16)
            for e in range(8):
                sent_ref[place_of(8 * c + e, FIRST[0]), pl.ds(t * SLICE, SLICE)] = tile[e * SLICE : (e + 1) * SLICE]
        sums.append(split3(total))
    rows = [sums[c][p].astype(F32) for p in range(3) for c in range(4)]
    for c in range(4):
        extra = jnp.concatenate([*rows, packed, packed, *masks[2 * c : 2 * c + 2]], axis=0).astype(BF16)
        for e in range(8):
            sent_ref[place_of(8 * c + e, FIRST[0]), pl.ds(2 * SLICE, SLICE)] = extra


def slices(mask, weights):
    return pl.pallas_call(
        slice_kernel,
        out_shape=jax.ShapeDtypeStruct((ROWS, 3 * SLICE, TILE), BF16),
        in_specs=[SMEM, VMEM],
        out_specs=VMEM,
        name="slices",
    )(mask, weights)


def panel_kernel(mask_ref, w_ref, panel_ref):
    for c in range(4):
        cols = pl.ds(c * TILE, TILE)
        masks = []
        for t in range(2):
            on = mask_ref[t, c].astype(F32)
            masks.append(jnp.full((1, TILE), on, F32))
            tile = w_ref[pl.ds(t * TILE, TILE), cols].astype(F32) * (on * UNIT)
            panel_ref[pl.ds(t * TILE, TILE), cols] = tile.astype(jnp.int32).astype(I16)
        rows = jnp.concatenate([*masks, jnp.zeros((6, TILE), F32)], axis=0)
        panel_ref[pl.ds(2 * TILE, 8), cols] = rows.astype(jnp.int32).astype(I16)


def fixed_panel(mask, weights):
    return pl.pallas_call(
        panel_kernel,
        out_shape=pltpu.VMEM((2 * TILE + 8, 4 * TILE), I16),
        in_specs=[SMEM, VMEM],
        out_specs=VMEM,
        name="panel",
    )(mask, weights)


def pack_kernel(core_ref, panel_ref, other_ref, packed_ref):
    core = core_ref[0]
    lane = lax.broadcasted_iota(jnp.int32, (1, TILE), 1)

    def both(rows, q):
        cols = pl.ds((q % 4) * TILE, TILE)
        mine, other = panel_ref[rows, cols].astype(jnp.int32), other_ref[rows, cols].astype(jnp.int32)
        return jnp.where(core == q // 4, mine, other)

    count = jnp.zeros((1, TILE), jnp.int32)
    meta = jnp.zeros((1, TILE), jnp.int32)
    slots = []
    for t in range(2):
        for q in range(8):
            on = both(pl.ds(2 * TILE, 8), q)[t : t + 1]
            slot = jnp.where(on > 0, count, -1)
            count = count + on
            slots.append(slot)
            meta = jnp.where(lane == 8 * t + q, slot, meta)
    for s in range(SLOTS):
        kept = jnp.zeros((HALF, TILE), jnp.int32)
        for t in range(2):
            rows = pl.ds(pl.multiple_of(t * TILE + core * HALF, HALF), HALF)
            for q in range(8):
                kept = jnp.where(slots[8 * t + q] == s, both(rows, q), kept)
        packed_ref[pl.ds(s * HALF, HALF)] = kept.astype(I16)
    rows = jnp.concatenate([jnp.zeros((8, TILE), jnp.int32), meta, jnp.zeros((7, TILE), jnp.int32)], axis=0)
    packed_ref[pl.ds(DEGREE, 16)] = rows.astype(I16)


def pack(core, panel, other):
    return pl.pallas_call(
        pack_kernel,
        out_shape=pltpu.VMEM((PACKED, TILE), I16),
        in_specs=[SMEM, VMEM, VMEM],
        out_specs=VMEM,
        name="pack",
    )(core, near(panel), near(other))


def place_kernel(own_ref, got_ref, packed_ref, placed_ref, full_ref, ids_ref, slot_ref):
    total = jnp.zeros((SLICE, TILE), F32)
    masks, tiles = [], []
    for r in range(ROWS):
        extra = got_ref[place_of(r, FIRST[0]), pl.ds(2 * SLICE, SLICE)].astype(F32)
        total = total + extra
        tiles.append(extra[12:13])
        masks.append(extra[14:16])
    degree = total[0:4] + (total[4:8] + total[8:12])
    high = jnp.floor(degree * 16.0)
    low = (degree * 16.0 - high) * UNIT
    tiles = jnp.concatenate(tiles, axis=0)
    row = lax.broadcasted_iota(jnp.int32, (ROWS, TILE), 0)
    lower = lax.broadcasted_iota(jnp.int32, (ROWS, TILE), 1) // 4
    pair = tiles + jnp.where(lower == 0, pltpu.roll(tiles, TILE - 4, 1), pltpu.roll(tiles, 4, 1))
    above = lax.broadcasted_iota(jnp.int32, (ROWS, ROWS), 0) > lax.broadcasted_iota(jnp.int32, (ROWS, ROWS), 1)
    rank = jnp.dot(above.astype(BF16), pair.astype(BF16), preferred_element_type=F32)
    rank = rank + jnp.where(lower == 1, pltpu.roll(tiles, 4, 1), 0.0)
    kept_row = (2 * row + lower).astype(F32)
    for s in range(KEEP):
        hit = jnp.where((tiles > 0) & (rank == s) & (lower < 2), kept_row, 0.0)
        hit = jnp.sum(hit, axis=0, keepdims=True)
        ids_ref[pl.ds(s, 1)] = (hit + pltpu.roll(hit, TILE - 4, 1)).astype(jnp.int32)
    tiles = jnp.concatenate([tiles, jnp.zeros((TILE - ROWS, TILE), F32)], axis=0).astype(BF16)
    counts = lax.dot_general(
        jnp.ones((8, TILE), BF16), tiles, (((1,), (1,)), ((), ())), preferred_element_type=F32
    )
    meta = packed_ref[pl.ds(META, 8)].astype(jnp.int32).astype(F32)
    rows = jnp.concatenate([high, low, meta[0:1], counts[0:7]], axis=0)
    full_ref[pl.ds(0, DEGREE)] = packed_ref[pl.ds(0, DEGREE)]
    full_ref[pl.ds(DEGREE, 16)] = rows.astype(jnp.int32).astype(I16)
    there = jnp.concatenate(masks, axis=0)
    above = lax.broadcasted_iota(jnp.int32, (64, 64), 0) > lax.broadcasted_iota(jnp.int32, (64, 64), 1)
    rank = jnp.dot(above.astype(BF16), there.astype(BF16), preferred_element_type=F32)
    slot_ref[...] = jnp.where(there > 0, rank, -1.0)
    own = own_ref[0]
    mine = jnp.zeros((1, TILE), F32)
    for c in range(4):
        mine = jnp.where(own == c, degree[c : c + 1], mine)
    kept = [jnp.zeros((SLICE, TILE), F32) for _ in range(KEEP)]
    for k in range(64):
        tile = got_ref[place_of(k // 2, FIRST[0]), pl.ds((k % 2) * SLICE, SLICE)].astype(F32)
        slot = jnp.broadcast_to(slot_ref[pl.ds(k, 1)], (SLICE, TILE))
        for s in range(KEEP):
            kept[s] = jnp.where(slot == s, tile, kept[s])
    for s in range(KEEP):
        tile = (kept[s] / mine).astype(BF16)
        for r in range(ROWS):
            placed_ref[r, s] = tile


def place(own, got, packed):
    return pl.pallas_call(
        place_kernel,
        out_shape=(
            pltpu.VMEM((ROWS, KEEP, SLICE, TILE), BF16),
            pltpu.VMEM((PACKED, TILE), I16),
            jax.ShapeDtypeStruct((KEEP, TILE), jnp.int32),
        ),
        in_specs=[SMEM, VMEM, VMEM],
        out_specs=(VMEM, VMEM, VMEM),
        scratch_shapes=[pltpu.VMEM((64, TILE), F32)],
        name="place",
    )(own, near(got), near(packed))


def expand_kernel(dense, ids_ref, slots_ref, full_ref, *refs):
    panel_ref = refs[0] if dense else None
    right_ref, out_ref, mass_ref, most_ref, inverse_ref = refs[-5:]
    most = jnp.zeros((8, TILE), jnp.int32)
    for z in range(NZ):
        held = jnp.zeros((8, TILE), jnp.int32)
        for col in range(NC * z, NC * z + NC):
            rows = full_ref[col, pl.ds(DEGREE, 16)].astype(jnp.int32)
            parts = rows[0:8].astype(F32)
            inverse_ref[col] = (16.0 / UNIT) / (parts[0:4] + parts[4:8] / UNIT)
            held = held + rows[8:16]
        most = jnp.maximum(most, held)
    most_ref[0] = jnp.max(most[1:2, :ROWS])
    for c in range(4):
        cols = pl.ds(c * TILE, TILE)
        total = jnp.zeros((2 * TILE, TILE), F32)
        for pair in range(KEEP // 2):
            lefts, rights = [], []
            for s in (2 * pair, 2 * pair + 1):
                k = ids_ref[s, c]
                inverse = inverse_ref[k // 4, pl.ds(k % 4, 1), :]
                if dense:
                    inside = pl.ds(pl.multiple_of((k % 4) * TILE, TILE), TILE)
                    left = panel_ref[k // 4, pl.ds(0, 2 * TILE), inside].astype(jnp.int32).astype(F32)
                    lefts.append((left * inverse).astype(BF16))
                else:
                    parts = []
                    for t in range(2):
                        slot = slots_ref[k // 8, 8 * t + k % 8]
                        start = pl.multiple_of(jnp.maximum(slot, 0) * HALF, HALF)
                        scaled = jnp.where(slot >= 0, inverse, 0.0)
                        for core in range(NC):
                            part = full_ref[(k // 8) * NC + core, pl.ds(start, HALF)].astype(jnp.int32)
                            parts.append((part.astype(F32) * scaled).astype(BF16))
                    lefts.append(jnp.concatenate(parts, axis=0))
                rights.extend(right_ref[place_of(8 * c + e, FIRST[1]), s] for e in range(8))
            total = total + jnp.dot(
                jnp.concatenate(lefts, axis=1),
                jnp.concatenate(rights, axis=0),
                preferred_element_type=F32,
            )
        total = total * total
        out_ref[:, cols] = total
        part = jnp.sum(total, axis=0, keepdims=True)
        for r in range(ROWS):
            mass_ref[r, :, cols] = part


def expand(ids, slots, full, *panels_and_right):
    dense = len(panels_and_right) == 2
    return pl.pallas_call(
        functools.partial(expand_kernel, dense),
        out_shape=(
            pltpu.VMEM((2 * TILE, 4 * TILE), F32),
            jax.ShapeDtypeStruct((ROWS, 1, 4 * TILE), F32),
            jax.ShapeDtypeStruct((1,), jnp.int32),
        ),
        in_specs=[SMEM, SMEM] + [VMEM] * (1 + len(panels_and_right)),
        out_specs=(VMEM, VMEM, SMEM),
        scratch_shapes=[pltpu.VMEM((NZ * NC, 4, TILE), F32)],
        compiler_params=LIMIT,
        name="expand_dense" if dense else "expand",
    )(ids, slots, full, *panels_and_right)


def scale_kernel(inflated_ref, mass_ref, flow_ref):
    mass = jnp.sum(mass_ref[...], axis=0)
    flow_ref[...] = inflated_ref[...] * (64.0 * TILE / mass)


def scale(inflated, mass):
    return pl.pallas_call(
        scale_kernel,
        out_shape=pltpu.HBM((2 * TILE, 4 * TILE), F32),
        in_specs=[VMEM, VMEM],
        out_specs=VMEM,
        name="scale",
    )(near(inflated), near(mass))


def on_device(weights, tile_mask):
    got = exchange(slices(tile_mask, weights), FIRST[0])
    panel = fixed_panel(tile_mask, weights)
    other = lax.ppermute(panel, "core", [(0, 1), (1, 0)])
    packed = pack(lax.axis_index("core").reshape(1), panel, other)
    own = (lax.axis_index("row") // 8).reshape(1)
    placed, full, ids = place(own, got, packed)
    right = exchange(placed, FIRST[1])
    full = lax.all_gather(full, COL)
    slots = full[::2, META, :16].astype(jnp.int32)
    inflated, mass, most = expand(ids, slots, full, right)
    mass = exchange(mass, FIRST[2])

    def overfull():
        inflated, mass, _ = expand(ids, slots, full, lax.all_gather(panel, COL), right)
        return scale(inflated, exchange(mass, FIRST[2]))

    return lax.cond(most[0] > SLOTS, overfull, lambda: scale(inflated, mass))


def solution(mesh):
    split = Mesh(mesh.devices.reshape(ROWS, NZ, NC), ("row", "z", "core"))
    placed = P("row", COL)
    return jax.shard_map(
        on_device, mesh=split, in_specs=(placed, placed), out_specs=placed, check_vma=False
    )
```

```python
import functools

import jax
import jax.numpy as jnp
from jax import lax
from jax.experimental import pallas as pl
from jax.experimental.pallas import tpu as pltpu
from jax.sharding import Mesh, PartitionSpec as P

KEEP = 8
TILE = 128
SLICE = 16
NY, NX, NZ, NC = 8, 4, 8, 2
ROWS = NY * NX
FIRST = ((4, 2), (2, 1), (4, 2))
F32, BF16, I16 = jnp.float32, jnp.bfloat16, jnp.int16
UNIT = 16384.0
SLOTS = 9
HALF = TILE // 2
DEGREE = SLOTS * HALF
META = DEGREE + 8
PACKED = META + 8
COL = ("z", "core")
LIMIT = pltpu.CompilerParams(vmem_limit_bytes=24 * 2**20)
VMEM = pl.BlockSpec(memory_space=pltpu.VMEM)
SMEM = pl.BlockSpec(memory_space=pltpu.SMEM)


def row_at(place, first):
    return (place // NX + first[0]) % NY * NX + (place + first[1]) % NX


def place_of(row, first):
    return row_at(row, (-first[0], -first[1]))


def exchange(blocks, first):
    group = [row_at(place, first) for place in range(ROWS)]
    return lax.all_to_all(
        blocks, "row", split_axis=0, concat_axis=0, tiled=True, axis_index_groups=[group]
    )


def near(x):
    return pltpu.with_memory_space_constraint(x, pltpu.VMEM)


def split3(v):
    parts = []
    for _ in range(3):
        part = v.astype(BF16)
        parts.append(part)
        v = v - part.astype(F32)
    return parts


def slice_kernel(mask_ref, w_ref, sent_ref):
    lane = lax.broadcasted_iota(jnp.int32, (1, TILE), 1)
    packed = jnp.zeros((1, TILE), F32)
    sums, masks = [], []
    for c in range(4):
        total = jnp.zeros((1, TILE), F32)
        for t in range(2):
            on = mask_ref[t, c].astype(F32)
            masks.append(jnp.full((1, TILE), on, F32))
            packed = jnp.where(lane == t * 4 + c, on, packed)
            tile = w_ref[pl.ds(t * TILE, TILE), pl.ds(c * TILE, TILE)].astype(F32) * on
            total = total + jnp.sum(tile, axis=0, keepdims=True)
            tile = tile.astype(BF16)
            for e in range(8):
                sent_ref[place_of(8 * c + e, FIRST[0]), pl.ds(t * SLICE, SLICE)] = tile[e * SLICE : (e + 1) * SLICE]
        sums.append(split3(total))
    rows = [sums[c][p].astype(F32) for p in range(3) for c in range(4)]
    for c in range(4):
        extra = jnp.concatenate([*rows, packed, packed, *masks[2 * c : 2 * c + 2]], axis=0).astype(BF16)
        for e in range(8):
            sent_ref[place_of(8 * c + e, FIRST[0]), pl.ds(2 * SLICE, SLICE)] = extra


def slices(mask, weights):
    return pl.pallas_call(
        slice_kernel,
        out_shape=jax.ShapeDtypeStruct((ROWS, 3 * SLICE, TILE), BF16),
        in_specs=[SMEM, VMEM],
        out_specs=VMEM,
        name="slices",
    )(mask, weights)


def panel_kernel(mask_ref, w_ref, panel_ref):
    for c in range(4):
        cols = pl.ds(c * TILE, TILE)
        masks = []
        for t in range(2):
            on = mask_ref[t, c].astype(F32)
            masks.append(jnp.full((1, TILE), on, F32))
            tile = w_ref[pl.ds(t * TILE, TILE), cols].astype(F32) * (on * UNIT)
            panel_ref[pl.ds(t * TILE, TILE), cols] = tile.astype(jnp.int32).astype(I16)
        rows = jnp.concatenate([*masks, jnp.zeros((6, TILE), F32)], axis=0)
        panel_ref[pl.ds(2 * TILE, 8), cols] = rows.astype(jnp.int32).astype(I16)


def fixed_panel(mask, weights):
    return pl.pallas_call(
        panel_kernel,
        out_shape=pltpu.VMEM((2 * TILE + 8, 4 * TILE), I16),
        in_specs=[SMEM, VMEM],
        out_specs=VMEM,
        name="panel",
    )(mask, weights)


def pack_kernel(core_ref, panel_ref, other_ref, packed_ref):
    core = core_ref[0]
    lane = lax.broadcasted_iota(jnp.int32, (1, TILE), 1)

    def both(rows, q):
        cols = pl.ds((q % 4) * TILE, TILE)
        mine, other = panel_ref[rows, cols].astype(jnp.int32), other_ref[rows, cols].astype(jnp.int32)
        return jnp.where(core == q // 4, mine, other)

    count = jnp.zeros((1, TILE), jnp.int32)
    meta = jnp.zeros((1, TILE), jnp.int32)
    slots = []
    for t in range(2):
        for q in range(8):
            on = both(pl.ds(2 * TILE, 8), q)[t : t + 1]
            slot = jnp.where(on > 0, count, -1)
            count = count + on
            slots.append(slot)
            meta = jnp.where(lane == 8 * t + q, slot, meta)
    for s in range(SLOTS):
        kept = jnp.zeros((HALF, TILE), jnp.int32)
        for t in range(2):
            rows = pl.ds(pl.multiple_of(t * TILE + core * HALF, HALF), HALF)
            for q in range(8):
                kept = jnp.where(slots[8 * t + q] == s, both(rows, q), kept)
        packed_ref[pl.ds(s * HALF, HALF)] = kept.astype(I16)
    rows = jnp.concatenate([jnp.zeros((8, TILE), jnp.int32), meta, jnp.zeros((7, TILE), jnp.int32)], axis=0)
    packed_ref[pl.ds(DEGREE, 16)] = rows.astype(I16)


def pack(core, panel, other):
    return pl.pallas_call(
        pack_kernel,
        out_shape=pltpu.VMEM((PACKED, TILE), I16),
        in_specs=[SMEM, VMEM, VMEM],
        out_specs=VMEM,
        name="pack",
    )(core, near(panel), near(other))


def place_kernel(own_ref, got_ref, packed_ref, placed_ref, full_ref, ids_ref, slot_ref):
    total = jnp.zeros((SLICE, TILE), F32)
    masks, tiles = [], []
    for r in range(ROWS):
        extra = got_ref[place_of(r, FIRST[0]), pl.ds(2 * SLICE, SLICE)].astype(F32)
        total = total + extra
        tiles.append(extra[12:13])
        masks.append(extra[14:16])
    degree = total[0:4] + (total[4:8] + total[8:12])
    high = jnp.floor(degree * 16.0)
    low = (degree * 16.0 - high) * UNIT
    tiles = jnp.concatenate(tiles, axis=0)
    row = lax.broadcasted_iota(jnp.int32, (ROWS, TILE), 0)
    lower = lax.broadcasted_iota(jnp.int32, (ROWS, TILE), 1) // 4
    pair = tiles + jnp.where(lower == 0, pltpu.roll(tiles, TILE - 4, 1), pltpu.roll(tiles, 4, 1))
    above = lax.broadcasted_iota(jnp.int32, (ROWS, ROWS), 0) > lax.broadcasted_iota(jnp.int32, (ROWS, ROWS), 1)
    rank = jnp.dot(above.astype(BF16), pair.astype(BF16), preferred_element_type=F32)
    rank = rank + jnp.where(lower == 1, pltpu.roll(tiles, 4, 1), 0.0)
    kept_row = (2 * row + lower).astype(F32)
    for s in range(KEEP):
        hit = jnp.where((tiles > 0) & (rank == s) & (lower < 2), kept_row, 0.0)
        hit = jnp.sum(hit, axis=0, keepdims=True)
        ids_ref[pl.ds(s, 1)] = (hit + pltpu.roll(hit, TILE - 4, 1)).astype(jnp.int32)
    tiles = jnp.concatenate([tiles, jnp.zeros((TILE - ROWS, TILE), F32)], axis=0).astype(BF16)
    counts = lax.dot_general(
        jnp.ones((8, TILE), BF16), tiles, (((1,), (1,)), ((), ())), preferred_element_type=F32
    )
    meta = packed_ref[pl.ds(META, 8)].astype(jnp.int32).astype(F32)
    rows = jnp.concatenate([high, low, meta[0:1], counts[0:7]], axis=0)
    full_ref[pl.ds(0, DEGREE)] = packed_ref[pl.ds(0, DEGREE)]
    full_ref[pl.ds(DEGREE, 16)] = rows.astype(jnp.int32).astype(I16)
    there = jnp.concatenate(masks, axis=0)
    above = lax.broadcasted_iota(jnp.int32, (64, 64), 0) > lax.broadcasted_iota(jnp.int32, (64, 64), 1)
    rank = jnp.dot(above.astype(BF16), there.astype(BF16), preferred_element_type=F32)
    slot_ref[...] = jnp.where(there > 0, rank, -1.0)
    own = own_ref[0]
    mine = jnp.zeros((1, TILE), F32)
    for c in range(4):
        mine = jnp.where(own == c, degree[c : c + 1], mine)
    kept = [jnp.zeros((SLICE, TILE), F32) for _ in range(KEEP)]
    for k in range(64):
        tile = got_ref[place_of(k // 2, FIRST[0]), pl.ds((k % 2) * SLICE, SLICE)].astype(F32)
        slot = jnp.broadcast_to(slot_ref[pl.ds(k, 1)], (SLICE, TILE))
        for s in range(KEEP):
            kept[s] = jnp.where(slot == s, tile, kept[s])
    for s in range(KEEP):
        tile = (kept[s] / mine).astype(BF16)
        for r in range(ROWS):
            placed_ref[r, s] = tile


def place(own, got, packed):
    return pl.pallas_call(
        place_kernel,
        out_shape=(
            pltpu.VMEM((ROWS, KEEP, SLICE, TILE), BF16),
            pltpu.VMEM((PACKED, TILE), I16),
            jax.ShapeDtypeStruct((KEEP, TILE), jnp.int32),
        ),
        in_specs=[SMEM, VMEM, VMEM],
        out_specs=(VMEM, VMEM, VMEM),
        scratch_shapes=[pltpu.VMEM((64, TILE), F32)],
        name="place",
    )(own, near(got), near(packed))


def expand_kernel(dense, ids_ref, slots_ref, full_ref, *refs):
    panel_ref = refs[0] if dense else None
    right_ref, out_ref, mass_ref, most_ref, inverse_ref = refs[-5:]
    most = jnp.zeros((8, TILE), jnp.int32)
    for z in range(NZ):
        held = jnp.zeros((8, TILE), jnp.int32)
        for col in range(NC * z, NC * z + NC):
            rows = full_ref[col, pl.ds(DEGREE, 16)].astype(jnp.int32)
            parts = rows[0:8].astype(F32)
            inverse_ref[col] = (16.0 / UNIT) / (parts[0:4] + parts[4:8] / UNIT)
            held = held + rows[8:16]
        most = jnp.maximum(most, held)
    most_ref[0] = jnp.max(most[1:2, :ROWS])
    for c in range(4):
        cols = pl.ds(c * TILE, TILE)
        total = jnp.zeros((2 * TILE, TILE), F32)
        for pair in range(KEEP // 2):
            lefts, rights = [], []
            for s in (2 * pair, 2 * pair + 1):
                k = ids_ref[s, c]
                inverse = inverse_ref[k // 4, pl.ds(k % 4, 1), :]
                if dense:
                    inside = pl.ds(pl.multiple_of((k % 4) * TILE, TILE), TILE)
                    left = panel_ref[k // 4, pl.ds(0, 2 * TILE), inside].astype(jnp.int32).astype(F32)
                    lefts.append((left * inverse).astype(BF16))
                else:
                    parts = []
                    for t in range(2):
                        slot = slots_ref[k // 8, 8 * t + k % 8]
                        start = pl.multiple_of(jnp.clip(slot, 0, SLOTS - 1) * HALF, HALF)
                        scaled = jnp.where(slot >= 0, inverse, 0.0)
                        for core in range(NC):
                            part = full_ref[(k // 8) * NC + core, pl.ds(start, HALF)].astype(jnp.int32)
                            parts.append((part.astype(F32) * scaled).astype(BF16))
                    lefts.append(jnp.concatenate(parts, axis=0))
                rights.extend(right_ref[place_of(8 * c + e, FIRST[1]), s] for e in range(8))
            total = total + jnp.dot(
                jnp.concatenate(lefts, axis=1),
                jnp.concatenate(rights, axis=0),
                preferred_element_type=F32,
            )
        total = total * total
        out_ref[:, cols] = total
        part = jnp.sum(total, axis=0, keepdims=True)
        for r in range(ROWS):
            mass_ref[r, :, cols] = part


def expand(ids, slots, full, *panels_and_right):
    dense = len(panels_and_right) == 2
    return pl.pallas_call(
        functools.partial(expand_kernel, dense),
        out_shape=(
            pltpu.VMEM((2 * TILE, 4 * TILE), F32),
            jax.ShapeDtypeStruct((ROWS, 1, 4 * TILE), F32),
            jax.ShapeDtypeStruct((1,), jnp.int32),
        ),
        in_specs=[SMEM, SMEM] + [VMEM] * (1 + len(panels_and_right)),
        out_specs=(VMEM, VMEM, SMEM),
        scratch_shapes=[pltpu.VMEM((NZ * NC, 4, TILE), F32)],
        compiler_params=LIMIT,
        name="expand_dense" if dense else "expand",
    )(ids, slots, full, *panels_and_right)


def scale_kernel(inflated_ref, mass_ref, flow_ref):
    mass = jnp.sum(mass_ref[...], axis=0)
    flow_ref[...] = inflated_ref[...] * (64.0 * TILE / mass)


def scale(inflated, mass):
    return pl.pallas_call(
        scale_kernel,
        out_shape=pltpu.HBM((2 * TILE, 4 * TILE), F32),
        in_specs=[VMEM, VMEM],
        out_specs=VMEM,
        name="scale",
    )(near(inflated), near(mass))


def on_device(weights, tile_mask):
    got = exchange(slices(tile_mask, weights), FIRST[0])
    panel = fixed_panel(tile_mask, weights)
    other = lax.ppermute(panel, "core", [(0, 1), (1, 0)])
    packed = pack(lax.axis_index("core").reshape(1), panel, other)
    own = (lax.axis_index("row") // 8).reshape(1)
    placed, full, ids = place(own, got, packed)
    right = exchange(placed, FIRST[1])
    full = lax.all_gather(full, COL)
    slots = full[::2, META, :16].astype(jnp.int32)
    inflated, mass, most = expand(ids, slots, full, right)
    mass = exchange(mass, FIRST[2])

    def overfull():
        inflated, mass, _ = expand(ids, slots, full, lax.all_gather(panel, COL), right)
        return scale(inflated, exchange(mass, FIRST[2]))

    return lax.cond(most[0] > SLOTS, overfull, lambda: scale(inflated, mass))


def solution(mesh):
    split = Mesh(mesh.devices.reshape(ROWS, NZ, NC), ("row", "z", "core"))
    placed = P("row", COL)
    return jax.shard_map(
        on_device, mesh=split, in_specs=(placed, placed), out_specs=placed, check_vma=False
    )
```

```python
import functools

import jax
import jax.numpy as jnp
from jax import lax
from jax.experimental import pallas as pl
from jax.experimental.pallas import tpu as pltpu
from jax.sharding import PartitionSpec as P

KEEP = 8
TILE = 128
SLICE = 16
NY, NX, NZ, NC = 8, 4, 8, 2
ROWS = NY * NX
FIRST = ((4, 2), (2, 1), (4, 2))
FIRST_Z = 4
F32, BF16, I16 = jnp.float32, jnp.bfloat16, jnp.int16
UNIT = 16384.0
SLOTS = 9
HALF = TILE // 2
DEGREE = SLOTS * HALF
META = DEGREE + 8
PACKED = META + 8
COLS = NZ * NC
LIMIT = pltpu.CompilerParams(vmem_limit_bytes=24 * 2**20)
VMEM = pl.BlockSpec(memory_space=pltpu.VMEM)
SMEM = pl.BlockSpec(memory_space=pltpu.SMEM)


def row_at(place, first):
    return (place // NX + first[0]) % NY * NX + (place + first[1]) % NX


def place_of(row, first):
    return row_at(row, (-first[0], -first[1]))


def exchange(blocks, first):
    group = [row_at(place, first) for place in range(ROWS)]
    return lax.all_to_all(
        blocks, "row", split_axis=0, concat_axis=0, tiled=True, axis_index_groups=[group]
    )


def near(x):
    return pltpu.with_memory_space_constraint(x, pltpu.VMEM)


def split3(v):
    parts = []
    for _ in range(3):
        part = v.astype(BF16)
        parts.append(part)
        v = v - part.astype(F32)
    return parts


def slice_kernel(mask_ref, w_ref, sent_ref):
    lane = lax.broadcasted_iota(jnp.int32, (1, TILE), 1)
    packed = jnp.zeros((1, TILE), F32)
    sums, masks = [], []
    for c in range(4):
        total = jnp.zeros((1, TILE), F32)
        for t in range(2):
            on = mask_ref[t, c].astype(F32)
            masks.append(jnp.full((1, TILE), on, F32))
            packed = jnp.where(lane == t * 4 + c, on, packed)
            tile = w_ref[pl.ds(t * TILE, TILE), pl.ds(c * TILE, TILE)].astype(F32) * on
            total = total + jnp.sum(tile, axis=0, keepdims=True)
            tile = tile.astype(BF16)
            for e in range(8):
                sent_ref[place_of(8 * c + e, FIRST[0]), pl.ds(t * SLICE, SLICE)] = tile[e * SLICE : (e + 1) * SLICE]
        sums.append(split3(total))
    rows = [sums[c][p].astype(F32) for p in range(3) for c in range(4)]
    for c in range(4):
        extra = jnp.concatenate([*rows, packed, packed, *masks[2 * c : 2 * c + 2]], axis=0).astype(BF16)
        for e in range(8):
            sent_ref[place_of(8 * c + e, FIRST[0]), pl.ds(2 * SLICE, SLICE)] = extra


def slices(mask, weights):
    return pl.pallas_call(
        slice_kernel,
        out_shape=jax.ShapeDtypeStruct((ROWS, 3 * SLICE, TILE), BF16),
        in_specs=[SMEM, VMEM],
        out_specs=VMEM,
        name="slices",
    )(mask, weights)


def panel_kernel(mask_ref, w_ref, panel_ref):
    for c in range(4):
        cols = pl.ds(c * TILE, TILE)
        masks = []
        for t in range(2):
            on = mask_ref[t, c].astype(F32)
            masks.append(jnp.full((1, TILE), on, F32))
            tile = w_ref[pl.ds(t * TILE, TILE), cols].astype(F32) * (on * UNIT)
            panel_ref[pl.ds(t * TILE, TILE), cols] = tile.astype(jnp.int32).astype(I16)
        rows = jnp.concatenate([*masks, jnp.zeros((6, TILE), F32)], axis=0)
        panel_ref[pl.ds(2 * TILE, 8), cols] = rows.astype(jnp.int32).astype(I16)


def fixed_panel(mask, weights):
    return pl.pallas_call(
        panel_kernel,
        out_shape=pltpu.VMEM((2 * TILE + 8, 4 * TILE), I16),
        in_specs=[SMEM, VMEM],
        out_specs=VMEM,
        name="panel",
    )(mask, weights)


def pack_kernel(core_ref, panel_ref, other_ref, packed_ref):
    core = core_ref[0]
    lane = lax.broadcasted_iota(jnp.int32, (1, TILE), 1)

    def both(rows, q):
        cols = pl.ds((q % 4) * TILE, TILE)
        mine, other = panel_ref[rows, cols].astype(jnp.int32), other_ref[rows, cols].astype(jnp.int32)
        return jnp.where(core == q // 4, mine, other)

    count = jnp.zeros((1, TILE), jnp.int32)
    meta = jnp.zeros((1, TILE), jnp.int32)
    slots = []
    for t in range(2):
        for q in range(8):
            on = both(pl.ds(2 * TILE, 8), q)[t : t + 1]
            slot = jnp.where(on > 0, count, -1)
            count = count + on
            slots.append(slot)
            meta = jnp.where(lane == 8 * t + q, slot, meta)
    for s in range(SLOTS):
        kept = jnp.zeros((HALF, TILE), jnp.int32)
        for t in range(2):
            rows = pl.ds(pl.multiple_of(t * TILE + core * HALF, HALF), HALF)
            for q in range(8):
                kept = jnp.where(slots[8 * t + q] == s, both(rows, q), kept)
        packed_ref[pl.ds(s * HALF, HALF)] = kept.astype(I16)
    rows = jnp.concatenate([jnp.zeros((8, TILE), jnp.int32), meta, jnp.zeros((7, TILE), jnp.int32)], axis=0)
    packed_ref[pl.ds(DEGREE, 16)] = rows.astype(I16)


def pack(core, panel, other):
    return pl.pallas_call(
        pack_kernel,
        out_shape=pltpu.VMEM((PACKED, TILE), I16),
        in_specs=[SMEM, VMEM, VMEM],
        out_specs=VMEM,
        name="pack",
    )(core, near(panel), near(other))


def place_kernel(own_ref, got_ref, packed_ref, placed_ref, full_ref, ids_ref, slot_ref):
    total = jnp.zeros((SLICE, TILE), F32)
    masks, tiles = [], []
    for r in range(ROWS):
        extra = got_ref[place_of(r, FIRST[0]), pl.ds(2 * SLICE, SLICE)].astype(F32)
        total = total + extra
        tiles.append(extra[12:13])
        masks.append(extra[14:16])
    degree = total[0:4] + (total[4:8] + total[8:12])
    high = jnp.floor(degree * 16.0)
    low = (degree * 16.0 - high) * UNIT
    tiles = jnp.concatenate(tiles, axis=0)
    row = lax.broadcasted_iota(jnp.int32, (ROWS, TILE), 0)
    lower = lax.broadcasted_iota(jnp.int32, (ROWS, TILE), 1) // 4
    pair = tiles + jnp.where(lower == 0, pltpu.roll(tiles, TILE - 4, 1), pltpu.roll(tiles, 4, 1))
    above = lax.broadcasted_iota(jnp.int32, (ROWS, ROWS), 0) > lax.broadcasted_iota(jnp.int32, (ROWS, ROWS), 1)
    rank = jnp.dot(above.astype(BF16), pair.astype(BF16), preferred_element_type=F32)
    rank = rank + jnp.where(lower == 1, pltpu.roll(tiles, 4, 1), 0.0)
    kept_row = (2 * row + lower).astype(F32)
    for s in range(KEEP):
        hit = jnp.where((tiles > 0) & (rank == s) & (lower < 2), kept_row, 0.0)
        hit = jnp.sum(hit, axis=0, keepdims=True)
        ids_ref[pl.ds(s, 1)] = (hit + pltpu.roll(hit, TILE - 4, 1)).astype(jnp.int32)
    tiles = jnp.concatenate([tiles, jnp.zeros((TILE - ROWS, TILE), F32)], axis=0).astype(BF16)
    counts = lax.dot_general(
        jnp.ones((8, TILE), BF16), tiles, (((1,), (1,)), ((), ())), preferred_element_type=F32
    )
    meta = packed_ref[pl.ds(META, 8)].astype(jnp.int32).astype(F32)
    rows = jnp.concatenate([high, low, meta[0:1], counts[0:7]], axis=0)
    full_ref[pl.ds(0, DEGREE)] = packed_ref[pl.ds(0, DEGREE)]
    full_ref[pl.ds(DEGREE, 16)] = rows.astype(jnp.int32).astype(I16)
    there = jnp.concatenate(masks, axis=0)
    above = lax.broadcasted_iota(jnp.int32, (64, 64), 0) > lax.broadcasted_iota(jnp.int32, (64, 64), 1)
    rank = jnp.dot(above.astype(BF16), there.astype(BF16), preferred_element_type=F32)
    slot_ref[...] = jnp.where(there > 0, rank, -1.0)
    own = own_ref[0]
    mine = jnp.zeros((1, TILE), F32)
    for c in range(4):
        mine = jnp.where(own == c, degree[c : c + 1], mine)
    kept = [jnp.zeros((SLICE, TILE), F32) for _ in range(KEEP)]
    for k in range(64):
        tile = got_ref[place_of(k // 2, FIRST[0]), pl.ds((k % 2) * SLICE, SLICE)].astype(F32)
        slot = jnp.broadcast_to(slot_ref[pl.ds(k, 1)], (SLICE, TILE))
        for s in range(KEEP):
            kept[s] = jnp.where(slot == s, tile, kept[s])
    for s in range(KEEP):
        tile = (kept[s] / mine).astype(BF16)
        for r in range(ROWS):
            placed_ref[r, s] = tile


def place(own, got, packed):
    return pl.pallas_call(
        place_kernel,
        out_shape=(
            pltpu.VMEM((ROWS, KEEP, SLICE, TILE), BF16),
            pltpu.VMEM((PACKED, TILE), I16),
            jax.ShapeDtypeStruct((KEEP, TILE), jnp.int32),
        ),
        in_specs=[SMEM, VMEM, VMEM],
        out_specs=(VMEM, VMEM, VMEM),
        scratch_shapes=[pltpu.VMEM((64, TILE), F32)],
        name="place",
    )(own, near(got), near(packed))


def expand_kernel(dense, ids_ref, slots_ref, full_ref, *refs):
    panel_ref = refs[0] if dense else None
    right_ref, out_ref, mass_ref, most_ref, inverse_ref = refs[-5:]
    most = jnp.zeros((8, TILE), jnp.int32)
    for z in range(NZ):
        held = jnp.zeros((8, TILE), jnp.int32)
        for col in range(NC * z, NC * z + NC):
            rows = full_ref[col, pl.ds(DEGREE, 16)].astype(jnp.int32)
            parts = rows[0:8].astype(F32)
            inverse_ref[col] = (16.0 / UNIT) / (parts[0:4] + parts[4:8] / UNIT)
            held = held + rows[8:16]
        most = jnp.maximum(most, held)
    most_ref[0] = jnp.max(most[1:2, :ROWS])
    for c in range(4):
        cols = pl.ds(c * TILE, TILE)
        total = jnp.zeros((2 * TILE, TILE), F32)
        for pair in range(KEEP // 2):
            lefts, rights = [], []
            for s in (2 * pair, 2 * pair + 1):
                k = ids_ref[s, c]
                chip = (k // 8 + NZ - FIRST_Z) % NZ
                inverse = inverse_ref[NC * chip + 1 - k // 4 % NC, pl.ds(k % 4, 1), :]
                if dense:
                    inside = pl.ds(pl.multiple_of((k % 4) * TILE, TILE), TILE)
                    left = panel_ref[k // 4, pl.ds(0, 2 * TILE), inside].astype(jnp.int32).astype(F32)
                    lefts.append((left * inverse).astype(BF16))
                else:
                    parts = []
                    for t in range(2):
                        slot = slots_ref[chip, 8 * t + k % 8]
                        start = pl.multiple_of(jnp.clip(slot, 0, SLOTS - 1) * HALF, HALF)
                        scaled = jnp.where(slot >= 0, inverse, 0.0)
                        for core in range(NC):
                            part = full_ref[chip * NC + 1 - core, pl.ds(start, HALF)].astype(jnp.int32)
                            parts.append((part.astype(F32) * scaled).astype(BF16))
                    lefts.append(jnp.concatenate(parts, axis=0))
                rights.extend(right_ref[place_of(8 * c + e, FIRST[1]), s] for e in range(8))
            total = total + jnp.dot(
                jnp.concatenate(lefts, axis=1),
                jnp.concatenate(rights, axis=0),
                preferred_element_type=F32,
            )
        total = total * total
        out_ref[:, cols] = total
        part = jnp.sum(total, axis=0, keepdims=True)
        for r in range(ROWS):
            mass_ref[r, :, cols] = part


def expand(ids, slots, full, *panels_and_right):
    dense = len(panels_and_right) == 2
    return pl.pallas_call(
        functools.partial(expand_kernel, dense),
        out_shape=(
            pltpu.VMEM((2 * TILE, 4 * TILE), F32),
            jax.ShapeDtypeStruct((ROWS, 1, 4 * TILE), F32),
            jax.ShapeDtypeStruct((1,), jnp.int32),
        ),
        in_specs=[SMEM, SMEM] + [VMEM] * (1 + len(panels_and_right)),
        out_specs=(VMEM, VMEM, SMEM),
        scratch_shapes=[pltpu.VMEM((NZ * NC, 4, TILE), F32)],
        compiler_params=LIMIT,
        name="expand_dense" if dense else "expand",
    )(ids, slots, full, *panels_and_right)


def scale_kernel(inflated_ref, mass_ref, flow_ref):
    mass = jnp.sum(mass_ref[...], axis=0)
    flow_ref[...] = inflated_ref[...] * (64.0 * TILE / mass)


def scale(inflated, mass):
    return pl.pallas_call(
        scale_kernel,
        out_shape=pltpu.HBM((2 * TILE, 4 * TILE), F32),
        in_specs=[VMEM, VMEM],
        out_specs=VMEM,
        name="scale",
    )(near(inflated), near(mass))


def on_device(weights, tile_mask):
    got = exchange(slices(tile_mask, weights), FIRST[0])
    panel = fixed_panel(tile_mask, weights)
    other = lax.ppermute(panel, "col", [(col, col ^ 1) for col in range(COLS)])
    packed = pack((lax.axis_index("col") % NC).reshape(1), panel, other)
    own = (lax.axis_index("row") // 8).reshape(1)
    placed, full, ids = place(own, got, packed)
    right = exchange(placed, FIRST[1])
    group = [(col + NC * FIRST_Z) % COLS ^ 1 for col in range(COLS)]
    full = full.reshape(1, PACKED // 8, 8, TILE)
    full = lax.all_gather(full, "col", axis=0, tiled=True, axis_index_groups=[group])
    full = full.reshape(COLS, PACKED, TILE)
    slots = full[::2, META, :16].astype(jnp.int32)
    inflated, mass, most = expand(ids, slots, full, right)
    mass = exchange(mass, FIRST[2])

    def overfull():
        inflated, mass, _ = expand(ids, slots, full, lax.all_gather(panel, "col"), right)
        return scale(inflated, exchange(mass, FIRST[2]))

    return lax.cond(most[0] > SLOTS, overfull, lambda: scale(inflated, mass))


def solution(mesh):
    placed = P("row", "col")
    return jax.shard_map(
        on_device, mesh=mesh, in_specs=(placed, placed), out_specs=placed, check_vma=False
    )
```

```python
import functools

import jax
import jax.numpy as jnp
from jax import lax
from jax.experimental import pallas as pl
from jax.experimental.pallas import tpu as pltpu
from jax.sharding import PartitionSpec as P

KEEP = 8
TILE = 128
SLICE = 16
NY, NX, NZ, NC = 8, 4, 8, 2
ROWS = NY * NX
FIRST = ((4, 2), (2, 1), (4, 2))
FIRST_Z = 4
F32, BF16, I16 = jnp.float32, jnp.bfloat16, jnp.int16
UNIT = 16384.0
SLOTS = 8
HALF = TILE // 2
DEGREE = SLOTS * HALF
META = DEGREE + 8
PACKED = META + 8
COLS = NZ * NC
LIMIT = pltpu.CompilerParams(vmem_limit_bytes=24 * 2**20)
VMEM = pl.BlockSpec(memory_space=pltpu.VMEM)
SMEM = pl.BlockSpec(memory_space=pltpu.SMEM)


def row_at(place, first):
    return (place // NX + first[0]) % NY * NX + (place + first[1]) % NX


def place_of(row, first):
    return row_at(row, (-first[0], -first[1]))


def exchange(blocks, first):
    group = [row_at(place, first) for place in range(ROWS)]
    return lax.all_to_all(
        blocks, "row", split_axis=0, concat_axis=0, tiled=True, axis_index_groups=[group]
    )


def near(x):
    return pltpu.with_memory_space_constraint(x, pltpu.VMEM)


def split3(v):
    parts = []
    for _ in range(3):
        part = v.astype(BF16)
        parts.append(part)
        v = v - part.astype(F32)
    return parts


def slice_kernel(mask_ref, w_ref, sent_ref):
    lane = lax.broadcasted_iota(jnp.int32, (1, TILE), 1)
    packed = jnp.zeros((1, TILE), F32)
    sums, masks = [], []
    for c in range(4):
        total = jnp.zeros((1, TILE), F32)
        for t in range(2):
            on = mask_ref[t, c].astype(F32)
            masks.append(jnp.full((1, TILE), on, F32))
            packed = jnp.where(lane == t * 4 + c, on, packed)
            tile = w_ref[pl.ds(t * TILE, TILE), pl.ds(c * TILE, TILE)].astype(F32) * on
            total = total + jnp.sum(tile, axis=0, keepdims=True)
            tile = tile.astype(BF16)
            for e in range(8):
                sent_ref[place_of(8 * c + e, FIRST[0]), pl.ds(t * SLICE, SLICE)] = tile[e * SLICE : (e + 1) * SLICE]
        sums.append(split3(total))
    rows = [sums[c][p].astype(F32) for p in range(3) for c in range(4)]
    for c in range(4):
        extra = jnp.concatenate([*rows, packed, packed, *masks[2 * c : 2 * c + 2]], axis=0).astype(BF16)
        for e in range(8):
            sent_ref[place_of(8 * c + e, FIRST[0]), pl.ds(2 * SLICE, SLICE)] = extra


def slices(mask, weights):
    return pl.pallas_call(
        slice_kernel,
        out_shape=jax.ShapeDtypeStruct((ROWS, 3 * SLICE, TILE), BF16),
        in_specs=[SMEM, VMEM],
        out_specs=VMEM,
        name="slices",
    )(mask, weights)


def panel_kernel(mask_ref, w_ref, panel_ref):
    for c in range(4):
        cols = pl.ds(c * TILE, TILE)
        masks = []
        for t in range(2):
            on = mask_ref[t, c].astype(F32)
            masks.append(jnp.full((1, TILE), on, F32))
            tile = w_ref[pl.ds(t * TILE, TILE), cols].astype(F32) * (on * UNIT)
            panel_ref[pl.ds(t * TILE, TILE), cols] = tile.astype(jnp.int32).astype(I16)
        rows = jnp.concatenate([*masks, jnp.zeros((6, TILE), F32)], axis=0)
        panel_ref[pl.ds(2 * TILE, 8), cols] = rows.astype(jnp.int32).astype(I16)


def fixed_panel(mask, weights):
    return pl.pallas_call(
        panel_kernel,
        out_shape=pltpu.VMEM((2 * TILE + 8, 4 * TILE), I16),
        in_specs=[SMEM, VMEM],
        out_specs=VMEM,
        name="panel",
    )(mask, weights)


def pack_kernel(core_ref, panel_ref, other_ref, packed_ref):
    core = core_ref[0]
    lane = lax.broadcasted_iota(jnp.int32, (1, TILE), 1)

    def both(rows, q):
        cols = pl.ds((q % 4) * TILE, TILE)
        mine, other = panel_ref[rows, cols].astype(jnp.int32), other_ref[rows, cols].astype(jnp.int32)
        return jnp.where(core == q // 4, mine, other)

    count = jnp.zeros((1, TILE), jnp.int32)
    meta = jnp.zeros((1, TILE), jnp.int32)
    slots = []
    for t in range(2):
        for q in range(8):
            on = both(pl.ds(2 * TILE, 8), q)[t : t + 1]
            slot = jnp.where(on > 0, count, -1)
            count = count + on
            slots.append(slot)
            meta = jnp.where(lane == 8 * t + q, slot, meta)
    for s in range(SLOTS):
        kept = jnp.zeros((HALF, TILE), jnp.int32)
        for t in range(2):
            rows = pl.ds(pl.multiple_of(t * TILE + core * HALF, HALF), HALF)
            for q in range(8):
                kept = jnp.where(slots[8 * t + q] == s, both(rows, q), kept)
        packed_ref[pl.ds(s * HALF, HALF)] = kept.astype(I16)
    rows = jnp.concatenate([jnp.zeros((8, TILE), jnp.int32), meta, jnp.zeros((7, TILE), jnp.int32)], axis=0)
    packed_ref[pl.ds(DEGREE, 16)] = rows.astype(I16)


def pack(core, panel, other):
    return pl.pallas_call(
        pack_kernel,
        out_shape=pltpu.VMEM((PACKED, TILE), I16),
        in_specs=[SMEM, VMEM, VMEM],
        out_specs=VMEM,
        name="pack",
    )(core, near(panel), near(other))


def place_kernel(own_ref, got_ref, packed_ref, placed_ref, full_ref, ids_ref, slot_ref):
    total = jnp.zeros((SLICE, TILE), F32)
    masks, tiles = [], []
    for r in range(ROWS):
        extra = got_ref[place_of(r, FIRST[0]), pl.ds(2 * SLICE, SLICE)].astype(F32)
        total = total + extra
        tiles.append(extra[12:13])
        masks.append(extra[14:16])
    degree = total[0:4] + (total[4:8] + total[8:12])
    high = jnp.floor(degree * 16.0)
    low = (degree * 16.0 - high) * UNIT
    tiles = jnp.concatenate(tiles, axis=0)
    row = lax.broadcasted_iota(jnp.int32, (ROWS, TILE), 0)
    lower = lax.broadcasted_iota(jnp.int32, (ROWS, TILE), 1) // 4
    pair = tiles + jnp.where(lower == 0, pltpu.roll(tiles, TILE - 4, 1), pltpu.roll(tiles, 4, 1))
    above = lax.broadcasted_iota(jnp.int32, (ROWS, ROWS), 0) > lax.broadcasted_iota(jnp.int32, (ROWS, ROWS), 1)
    rank = jnp.dot(above.astype(BF16), pair.astype(BF16), preferred_element_type=F32)
    rank = rank + jnp.where(lower == 1, pltpu.roll(tiles, 4, 1), 0.0)
    kept_row = (2 * row + lower).astype(F32)
    for s in range(KEEP):
        hit = jnp.where((tiles > 0) & (rank == s) & (lower < 2), kept_row, 0.0)
        hit = jnp.sum(hit, axis=0, keepdims=True)
        ids_ref[pl.ds(s, 1)] = (hit + pltpu.roll(hit, TILE - 4, 1)).astype(jnp.int32)
    tiles = jnp.concatenate([tiles, jnp.zeros((TILE - ROWS, TILE), F32)], axis=0).astype(BF16)
    counts = lax.dot_general(
        jnp.ones((8, TILE), BF16), tiles, (((1,), (1,)), ((), ())), preferred_element_type=F32
    )
    meta = packed_ref[pl.ds(META, 8)].astype(jnp.int32).astype(F32)
    rows = jnp.concatenate([high, low, meta[0:1], counts[0:7]], axis=0)
    full_ref[pl.ds(0, DEGREE)] = packed_ref[pl.ds(0, DEGREE)]
    full_ref[pl.ds(DEGREE, 16)] = rows.astype(jnp.int32).astype(I16)
    there = jnp.concatenate(masks, axis=0)
    above = lax.broadcasted_iota(jnp.int32, (64, 64), 0) > lax.broadcasted_iota(jnp.int32, (64, 64), 1)
    rank = jnp.dot(above.astype(BF16), there.astype(BF16), preferred_element_type=F32)
    slot_ref[...] = jnp.where(there > 0, rank, -1.0)
    own = own_ref[0]
    mine = jnp.zeros((1, TILE), F32)
    for c in range(4):
        mine = jnp.where(own == c, degree[c : c + 1], mine)
    kept = [jnp.zeros((SLICE, TILE), F32) for _ in range(KEEP)]
    for k in range(64):
        tile = got_ref[place_of(k // 2, FIRST[0]), pl.ds((k % 2) * SLICE, SLICE)].astype(F32)
        slot = jnp.broadcast_to(slot_ref[pl.ds(k, 1)], (SLICE, TILE))
        for s in range(KEEP):
            kept[s] = jnp.where(slot == s, tile, kept[s])
    for s in range(KEEP):
        tile = (kept[s] / mine).astype(BF16)
        for r in range(ROWS):
            placed_ref[r, s] = tile


def place(own, got, packed):
    return pl.pallas_call(
        place_kernel,
        out_shape=(
            pltpu.VMEM((ROWS, KEEP, SLICE, TILE), BF16),
            pltpu.VMEM((PACKED, TILE), I16),
            jax.ShapeDtypeStruct((KEEP, TILE), jnp.int32),
        ),
        in_specs=[SMEM, VMEM, VMEM],
        out_specs=(VMEM, VMEM, VMEM),
        scratch_shapes=[pltpu.VMEM((64, TILE), F32)],
        name="place",
    )(own, near(got), near(packed))


def expand_kernel(dense, ids_ref, slots_ref, full_ref, *refs):
    panel_ref = refs[0] if dense else None
    right_ref, out_ref, mass_ref, most_ref, inverse_ref = refs[-5:]
    most = jnp.zeros((8, TILE), jnp.int32)
    for z in range(NZ):
        held = jnp.zeros((8, TILE), jnp.int32)
        for col in range(NC * z, NC * z + NC):
            rows = full_ref[col, pl.ds(DEGREE, 16)].astype(jnp.int32)
            parts = rows[0:8].astype(F32)
            inverse_ref[col] = (16.0 / UNIT) / (parts[0:4] + parts[4:8] / UNIT)
            held = held + rows[8:16]
        most = jnp.maximum(most, held)
    most_ref[0] = jnp.max(most[1:2, :ROWS])
    for c in range(4):
        cols = pl.ds(c * TILE, TILE)
        total = jnp.zeros((2 * TILE, TILE), F32)
        for pair in range(KEEP // 2):
            lefts, rights = [], []
            for s in (2 * pair, 2 * pair + 1):
                k = ids_ref[s, c]
                chip = (k // 8 + NZ - FIRST_Z) % NZ
                inverse = inverse_ref[NC * chip + 1 - k // 4 % NC, pl.ds(k % 4, 1), :]
                if dense:
                    inside = pl.ds(pl.multiple_of((k % 4) * TILE, TILE), TILE)
                    left = panel_ref[k // 4, pl.ds(0, 2 * TILE), inside].astype(jnp.int32).astype(F32)
                    lefts.append((left * inverse).astype(BF16))
                else:
                    parts = []
                    for t in range(2):
                        slot = slots_ref[chip, 8 * t + k % 8]
                        start = pl.multiple_of(jnp.clip(slot, 0, SLOTS - 1) * HALF, HALF)
                        scaled = jnp.where(slot >= 0, inverse, 0.0)
                        for core in range(NC):
                            part = full_ref[chip * NC + 1 - core, pl.ds(start, HALF)].astype(jnp.int32)
                            parts.append((part.astype(F32) * scaled).astype(BF16))
                    lefts.append(jnp.concatenate(parts, axis=0))
                rights.extend(right_ref[place_of(8 * c + e, FIRST[1]), s] for e in range(8))
            total = total + jnp.dot(
                jnp.concatenate(lefts, axis=1),
                jnp.concatenate(rights, axis=0),
                preferred_element_type=F32,
            )
        total = total * total
        out_ref[:, cols] = total
        part = jnp.sum(total, axis=0, keepdims=True)
        for r in range(ROWS):
            mass_ref[r, :, cols] = part


def expand(ids, slots, full, *panels_and_right):
    dense = len(panels_and_right) == 2
    return pl.pallas_call(
        functools.partial(expand_kernel, dense),
        out_shape=(
            pltpu.VMEM((2 * TILE, 4 * TILE), F32),
            jax.ShapeDtypeStruct((ROWS, 1, 4 * TILE), F32),
            jax.ShapeDtypeStruct((1,), jnp.int32),
        ),
        in_specs=[SMEM, SMEM] + [VMEM] * (1 + len(panels_and_right)),
        out_specs=(VMEM, VMEM, SMEM),
        scratch_shapes=[pltpu.VMEM((NZ * NC, 4, TILE), F32)],
        compiler_params=LIMIT,
        name="expand_dense" if dense else "expand",
    )(ids, slots, full, *panels_and_right)


def scale_kernel(inflated_ref, mass_ref, flow_ref):
    mass = jnp.sum(mass_ref[...], axis=0)
    flow_ref[...] = inflated_ref[...] * (64.0 * TILE / mass)


def scale(inflated, mass):
    return pl.pallas_call(
        scale_kernel,
        out_shape=pltpu.HBM((2 * TILE, 4 * TILE), F32),
        in_specs=[VMEM, VMEM],
        out_specs=VMEM,
        name="scale",
    )(near(inflated), near(mass))


def on_device(weights, tile_mask):
    got = exchange(slices(tile_mask, weights), FIRST[0])
    panel = fixed_panel(tile_mask, weights)
    other = lax.ppermute(panel, "col", [(col, col ^ 1) for col in range(COLS)])
    packed = pack((lax.axis_index("col") % NC).reshape(1), panel, other)
    own = (lax.axis_index("row") // 8).reshape(1)
    placed, full, ids = place(own, got, packed)
    right = exchange(placed, FIRST[1])
    group = [(col + NC * FIRST_Z) % COLS ^ 1 for col in range(COLS)]
    full = full.reshape(1, PACKED // 8, 8, TILE)
    full = lax.all_gather(full, "col", axis=0, tiled=True, axis_index_groups=[group])
    full = full.reshape(COLS, PACKED, TILE)
    slots = full[::2, META, :16].astype(jnp.int32)
    inflated, mass, most = expand(ids, slots, full, right)
    mass = exchange(mass, FIRST[2])

    def overfull():
        inflated, mass, _ = expand(ids, slots, full, lax.all_gather(panel, "col"), right)
        return scale(inflated, exchange(mass, FIRST[2]))

    return lax.cond(most[0] > SLOTS, overfull, lambda: scale(inflated, mass))


def solution(mesh):
    placed = P("row", "col")
    return jax.shard_map(
        on_device, mesh=mesh, in_specs=(placed, placed), out_specs=placed, check_vma=False
    )
```

```python
import functools

import jax
import jax.numpy as jnp
from jax import lax
from jax.experimental import pallas as pl
from jax.experimental.pallas import tpu as pltpu
from jax.sharding import PartitionSpec as P

KEEP = 8
TILE = 128
SLICE = 16
NY, NX, NZ, NC = 8, 4, 8, 2
ROWS = NY * NX
FIRST = ((4, 2), (2, 1), (4, 2))
FIRST_Z = 4
F32, BF16, I16 = jnp.float32, jnp.bfloat16, jnp.int16
UNIT = 16384.0
SLOTS = 8
HALF = TILE // 2
DEGREE = SLOTS * HALF
META = DEGREE + 8
PACKED = META + 8
COLS = NZ * NC
LIMIT = pltpu.CompilerParams(vmem_limit_bytes=24 * 2**20)
VMEM = pl.BlockSpec(memory_space=pltpu.VMEM)
SMEM = pl.BlockSpec(memory_space=pltpu.SMEM)


def row_at(place, first):
    return (place // NX + first[0]) % NY * NX + (place + first[1]) % NX


def place_of(row, first):
    return row_at(row, (-first[0], -first[1]))


def exchange(blocks, first):
    group = [row_at(place, first) for place in range(ROWS)]
    return lax.all_to_all(
        blocks, "row", split_axis=0, concat_axis=0, tiled=True, axis_index_groups=[group]
    )


def near(x):
    return pltpu.with_memory_space_constraint(x, pltpu.VMEM)


def split3(v):
    parts = []
    for _ in range(3):
        part = v.astype(BF16)
        parts.append(part)
        v = v - part.astype(F32)
    return parts


def slice_kernel(mask_ref, w_ref, sent_ref):
    lane = lax.broadcasted_iota(jnp.int32, (1, TILE), 1)
    packed = jnp.zeros((1, TILE), F32)
    sums, masks = [], []
    for c in range(4):
        total = jnp.zeros((1, TILE), F32)
        for t in range(2):
            on = mask_ref[t, c].astype(F32)
            masks.append(jnp.full((1, TILE), on, F32))
            packed = jnp.where(lane == t * 4 + c, on, packed)
            tile = w_ref[pl.ds(t * TILE, TILE), pl.ds(c * TILE, TILE)].astype(F32) * on
            total = total + jnp.sum(tile, axis=0, keepdims=True)
            tile = tile.astype(BF16)
            for e in range(8):
                sent_ref[place_of(8 * c + e, FIRST[0]), pl.ds(t * SLICE, SLICE)] = tile[e * SLICE : (e + 1) * SLICE]
        sums.append(split3(total))
    rows = [sums[c][p].astype(F32) for p in range(3) for c in range(4)]
    for c in range(4):
        extra = jnp.concatenate([*rows, packed, packed, *masks[2 * c : 2 * c + 2]], axis=0).astype(BF16)
        for e in range(8):
            sent_ref[place_of(8 * c + e, FIRST[0]), pl.ds(2 * SLICE, SLICE)] = extra


def slices(mask, weights):
    return pl.pallas_call(
        slice_kernel,
        out_shape=jax.ShapeDtypeStruct((ROWS, 3 * SLICE, TILE), BF16),
        in_specs=[SMEM, VMEM],
        out_specs=VMEM,
        name="slices",
    )(mask, weights)


def panel_kernel(mask_ref, w_ref, panel_ref):
    for c in range(4):
        cols = pl.ds(c * TILE, TILE)
        masks = []
        for t in range(2):
            on = mask_ref[t, c].astype(F32)
            masks.append(jnp.full((1, TILE), on, F32))
            tile = w_ref[pl.ds(t * TILE, TILE), cols].astype(F32) * (on * UNIT)
            panel_ref[pl.ds(t * TILE, TILE), cols] = tile.astype(jnp.int32).astype(I16)
        rows = jnp.concatenate([*masks, jnp.zeros((6, TILE), F32)], axis=0)
        panel_ref[pl.ds(2 * TILE, 8), cols] = rows.astype(jnp.int32).astype(I16)


def fixed_panel(mask, weights):
    return pl.pallas_call(
        panel_kernel,
        out_shape=pltpu.VMEM((2 * TILE + 8, 4 * TILE), I16),
        in_specs=[SMEM, VMEM],
        out_specs=VMEM,
        name="panel",
    )(mask, weights)


def pack_kernel(core_ref, panel_ref, other_ref, packed_ref):
    core = core_ref[0]
    lane = lax.broadcasted_iota(jnp.int32, (1, TILE), 1)

    def both(rows, q):
        cols = pl.ds((q % 4) * TILE, TILE)
        mine, other = panel_ref[rows, cols].astype(jnp.int32), other_ref[rows, cols].astype(jnp.int32)
        return jnp.where(core == q // 4, mine, other)

    count = jnp.zeros((1, TILE), jnp.int32)
    meta = jnp.zeros((1, TILE), jnp.int32)
    slots = []
    for t in range(2):
        for q in range(8):
            on = both(pl.ds(2 * TILE, 8), q)[t : t + 1]
            slot = jnp.where(on > 0, count, -1)
            count = count + on
            slots.append(slot)
            meta = jnp.where(lane == 8 * t + q, slot, meta)
    for s in range(SLOTS):
        kept = jnp.zeros((HALF, TILE), jnp.int32)
        for t in range(2):
            rows = pl.ds(pl.multiple_of(t * TILE + core * HALF, HALF), HALF)
            for q in range(8):
                kept = jnp.where(slots[8 * t + q] == s, both(rows, q), kept)
        packed_ref[pl.ds(s * HALF, HALF)] = kept.astype(I16)
    rows = jnp.concatenate([jnp.zeros((8, TILE), jnp.int32), meta, jnp.zeros((7, TILE), jnp.int32)], axis=0)
    packed_ref[pl.ds(DEGREE, 16)] = rows.astype(I16)


def pack(core, panel, other):
    return pl.pallas_call(
        pack_kernel,
        out_shape=pltpu.VMEM((PACKED, TILE), I16),
        in_specs=[SMEM, VMEM, VMEM],
        out_specs=VMEM,
        name="pack",
    )(core, near(panel), near(other))


def place_kernel(own_ref, got_ref, packed_ref, placed_ref, full_ref, ids_ref, slot_ref):
    total = jnp.zeros((SLICE, TILE), F32)
    masks, tiles = [], []
    for r in range(ROWS):
        extra = got_ref[place_of(r, FIRST[0]), pl.ds(2 * SLICE, SLICE)].astype(F32)
        total = total + extra
        tiles.append(extra[12:13])
        masks.append(extra[14:16])
    degree = total[0:4] + (total[4:8] + total[8:12])
    high = jnp.floor(degree * 16.0)
    low = (degree * 16.0 - high) * UNIT
    tiles = jnp.concatenate(tiles, axis=0)
    row = lax.broadcasted_iota(jnp.int32, (ROWS, TILE), 0)
    lower = lax.broadcasted_iota(jnp.int32, (ROWS, TILE), 1) // 4
    pair = tiles + jnp.where(lower == 0, pltpu.roll(tiles, TILE - 4, 1), pltpu.roll(tiles, 4, 1))
    above = lax.broadcasted_iota(jnp.int32, (ROWS, ROWS), 0) > lax.broadcasted_iota(jnp.int32, (ROWS, ROWS), 1)
    rank = jnp.dot(above.astype(BF16), pair.astype(BF16), preferred_element_type=F32)
    rank = rank + jnp.where(lower == 1, pltpu.roll(tiles, 4, 1), 0.0)
    kept_row = (2 * row + lower).astype(F32)
    for s in range(KEEP):
        hit = jnp.where((tiles > 0) & (rank == s) & (lower < 2), kept_row, 0.0)
        hit = jnp.sum(hit, axis=0, keepdims=True)
        ids_ref[pl.ds(s, 1)] = (hit + pltpu.roll(hit, TILE - 4, 1)).astype(jnp.int32)
    tiles = jnp.concatenate([tiles, jnp.zeros((TILE - ROWS, TILE), F32)], axis=0).astype(BF16)
    counts = lax.dot_general(
        jnp.ones((8, TILE), BF16), tiles, (((1,), (1,)), ((), ())), preferred_element_type=F32
    )
    meta = packed_ref[pl.ds(META, 8)].astype(jnp.int32).astype(F32)
    rows = jnp.concatenate([high, low, meta[0:1], counts[0:7]], axis=0)
    full_ref[pl.ds(0, DEGREE)] = packed_ref[pl.ds(0, DEGREE)]
    full_ref[pl.ds(DEGREE, 16)] = rows.astype(jnp.int32).astype(I16)
    there = jnp.concatenate(masks, axis=0)
    above = lax.broadcasted_iota(jnp.int32, (64, 64), 0) > lax.broadcasted_iota(jnp.int32, (64, 64), 1)
    rank = jnp.dot(above.astype(BF16), there.astype(BF16), preferred_element_type=F32)
    slot_ref[...] = jnp.where(there > 0, rank, -1.0)
    own = own_ref[0]
    mine = jnp.zeros((1, TILE), F32)
    for c in range(4):
        mine = jnp.where(own == c, degree[c : c + 1], mine)
    kept = [jnp.zeros((SLICE, TILE), F32) for _ in range(KEEP)]
    for k in range(64):
        tile = got_ref[place_of(k // 2, FIRST[0]), pl.ds((k % 2) * SLICE, SLICE)].astype(F32)
        slot = jnp.broadcast_to(slot_ref[pl.ds(k, 1)], (SLICE, TILE))
        for s in range(KEEP):
            kept[s] = jnp.where(slot == s, tile, kept[s])
    for s in range(KEEP):
        tile = (kept[s] / mine).astype(BF16)
        for r in range(ROWS):
            placed_ref[r, s] = tile


def place(own, got, packed):
    return pl.pallas_call(
        place_kernel,
        out_shape=(
            pltpu.VMEM((ROWS, KEEP, SLICE, TILE), BF16),
            pltpu.VMEM((PACKED, TILE), I16),
            jax.ShapeDtypeStruct((KEEP, TILE), jnp.int32),
        ),
        in_specs=[SMEM, VMEM, VMEM],
        out_specs=(VMEM, VMEM, VMEM),
        scratch_shapes=[pltpu.VMEM((64, TILE), F32)],
        name="place",
    )(own, near(got), near(packed))


def expand_kernel(dense, ids_ref, slots_ref, full_ref, *refs):
    panel_ref = refs[0] if dense else None
    right_ref, out_ref, mass_ref, most_ref, inverse_ref = refs[-5:]
    most = jnp.zeros((8, TILE), jnp.int32)
    for z in range(NZ):
        held = jnp.zeros((8, TILE), jnp.int32)
        for col in range(NC * z, NC * z + NC):
            rows = full_ref[col, pl.ds(DEGREE, 16)].astype(jnp.int32)
            parts = rows[0:8].astype(F32)
            inverse_ref[col] = (16.0 / UNIT) / (parts[0:4] + parts[4:8] / UNIT)
            held = held + rows[8:16]
        most = jnp.maximum(most, held)
    most_ref[0] = jnp.max(most[1:2, :ROWS])
    for c in range(4):
        cols = pl.ds(c * TILE, TILE)
        total = jnp.zeros((2 * TILE, TILE), F32)
        for pair in range(KEEP // 2):
            lefts, rights = [], []
            for s in (2 * pair, 2 * pair + 1):
                k = ids_ref[s, c]
                chip = (k // 8 + NZ - FIRST_Z) % NZ
                inverse = inverse_ref[NC * chip + 1 - k // 4 % NC, pl.ds(k % 4, 1), :]
                if dense:
                    inside = pl.ds(pl.multiple_of((k % 4) * TILE, TILE), TILE)
                    left = panel_ref[k // 4, pl.ds(0, 2 * TILE), inside].astype(jnp.int32).astype(F32)
                    lefts.append((left * inverse).astype(BF16))
                else:
                    parts = []
                    for t in range(2):
                        slot = slots_ref[chip, 8 * t + k % 8]
                        start = pl.multiple_of(jnp.clip(slot, 0, SLOTS - 1) * HALF, HALF)
                        scaled = jnp.where(slot >= 0, inverse, 0.0)
                        for core in range(NC):
                            part = full_ref[chip * NC + 1 - core, pl.ds(start, HALF)].astype(jnp.int32)
                            parts.append((part.astype(F32) * scaled).astype(BF16))
                    lefts.append(jnp.concatenate(parts, axis=0))
                rights.extend(right_ref[place_of(8 * c + e, FIRST[1]), s] for e in range(8))
            total = total + jnp.dot(
                jnp.concatenate(lefts, axis=1),
                jnp.concatenate(rights, axis=0),
                preferred_element_type=F32,
            )
        total = total * total
        out_ref[:, cols] = total
        part = jnp.sum(total, axis=0, keepdims=True)
        for r in range(ROWS):
            mass_ref[r, :, cols] = part


def expand(ids, slots, full, *panels_and_right):
    dense = len(panels_and_right) == 2
    return pl.pallas_call(
        functools.partial(expand_kernel, dense),
        out_shape=(
            pltpu.VMEM((2 * TILE, 4 * TILE), F32),
            jax.ShapeDtypeStruct((ROWS, 1, 4 * TILE), F32),
            jax.ShapeDtypeStruct((1,), jnp.int32),
        ),
        in_specs=[SMEM, SMEM] + [VMEM] * (1 + len(panels_and_right)),
        out_specs=(VMEM, VMEM, SMEM),
        scratch_shapes=[pltpu.VMEM((NZ * NC, 4, TILE), F32)],
        compiler_params=LIMIT,
        name="expand_dense" if dense else "expand",
    )(ids, slots, full, *panels_and_right)


def scale_kernel(inflated_ref, mass_ref, flow_ref):
    mass = jnp.sum(mass_ref[...], axis=0)
    flow_ref[...] = inflated_ref[...] * (64.0 * TILE / mass)


def scale(inflated, mass):
    return pl.pallas_call(
        scale_kernel,
        out_shape=pltpu.HBM((2 * TILE, 4 * TILE), F32),
        in_specs=[VMEM, VMEM],
        out_specs=VMEM,
        compiler_params=pltpu.CompilerParams(vmem_limit_bytes=57 * 2**20),
        name="scale",
    )(near(inflated), near(mass))


def on_device(weights, tile_mask):
    got = exchange(slices(tile_mask, weights), FIRST[0])
    panel = fixed_panel(tile_mask, weights)
    other = lax.ppermute(panel, "col", [(col, col ^ 1) for col in range(COLS)])
    packed = pack((lax.axis_index("col") % NC).reshape(1), panel, other)
    own = (lax.axis_index("row") // 8).reshape(1)
    placed, full, ids = place(own, got, packed)
    right = near(exchange(placed, FIRST[1]))
    group = [(col + NC * FIRST_Z) % COLS ^ 1 for col in range(COLS)]
    full = full.reshape(1, PACKED // 8, 8, TILE)
    full = lax.all_gather(full, "col", axis=0, tiled=True, axis_index_groups=[group])
    full = full.reshape(COLS, PACKED, TILE)
    slots = full[::2, META, :16].astype(jnp.int32)
    inflated, mass, most = expand(ids, slots, full, right)
    mass = exchange(mass, FIRST[2])

    def overfull():
        inflated, mass, _ = expand(ids, slots, full, lax.all_gather(panel, "col"), right)
        return scale(inflated, exchange(mass, FIRST[2]))

    return lax.cond(most[0] > SLOTS, overfull, lambda: scale(inflated, mass))


def solution(mesh):
    placed = P("row", "col")
    return jax.shard_map(
        on_device, mesh=mesh, in_specs=(placed, placed), out_specs=placed, check_vma=False
    )
```
